32 devices in a mesh: dp: 4 (over y, core), expert: 8 (over z, x).
Axes of the slice: x: 2, y: 2, z: 4, core: 2. Of those that a mesh axis runs over, the one named last changes fastest.
Arguments:
- tokens: bfloat16 [4096, 1024], P(('dp', 'expert')), may hold values from -6 to 6
- chosen_expert_index: int32 [4096, 6], P(('dp', 'expert')), may hold values from 0 to 7, as said below
- router_gate_weight: float32 [4096, 6], P(('dp', 'expert')), may hold values from 0.05 to 0.5
- output_gradient: bfloat16 [4096, 1024], P(('dp', 'expert')), may hold values from -0.15917969 to 0.15917969
- gate_weight_matrix: bfloat16 [8, 1024, 704], P('expert'), may hold values from -0.1875 to 0.1875
- up_weight: bfloat16 [8, 1024, 704], P('expert'), may hold values from -0.1875 to 0.1875
- down_weight: bfloat16 [8, 704, 1024], P('expert'), may hold values from -0.21875 to 0.21875
- adapter_down_maps: bfloat16 [8, 16, 704], P('expert'), may hold values from -0.21875 to 0.21875
- adapter_up_maps: bfloat16 [8, 16, 1024], P('expert'), may hold values from -1.5 to 1.5
Outputs:
- mixed: bfloat16 [4096, 1024], P(('dp', 'expert'))
- grad_in: bfloat16 [8, 16, 704], P('expert')
- grad_out: bfloat16 [8, 16, 1024], P('expert')
The draws below stay inside these ranges and needn't reach their ends.
Inputs may be any that keep to these rules, and one draw needn't show every extreme that they name: `chosen_expert_index`: each row names 6 different experts. In each aligned block of 128 rows (the rows of one device) no expert is named by more than 126 rows, and one and the same expert, drawn for the whole array, is named by exactly 126 rows of every block. Each row's experts are 6 neighbours in one circular order of all experts, drawn for the whole array.
All inputs are finite; a program needn't handle non-finite values.
Results may differ from the reference program's by a relative error of at most 0.0064.
Values may be sent and summed in bfloat16 or wider, within the bound.
A program may use at most 64 MiB of HBM per device.

```python
import math
import jax
import jax.numpy as jnp
from jax import lax

MODEL_FEATURES = 1024
HIDDEN_UNITS = 704
ADAPTER_DEPTH = 16
TOPK = 6
TOK_DEV = 128
ROUTED_EXPERTS = 8
TOKENS = 4096
HOT = 21
CAP = 126


def draw_chosen_expert_index(key, part):
    blocks = TOKENS // TOK_DEV
    others = ROUTED_EXPERTS - TOPK
    order_key, spread_keys = jax.random.split(jax.random.fold_in(key, 11))
    labels = jax.random.permutation(order_key, ROUTED_EXPERTS).astype(jnp.int32)
    position = jnp.arange(TOK_DEV, dtype=jnp.int32)
    offsets = jnp.arange(TOPK, dtype=jnp.int32)

    def one_block(block_key):
        shuffle_key, spread_key = jax.random.split(block_key)
        spread = TOPK + jax.random.permutation(spread_key, others).astype(jnp.int32)
        hot_start = position // HOT
        cold_index = jnp.maximum(position - TOPK * HOT, 0) % others
        cold_start = spread[cold_index]
        start_label = jnp.where(position < TOPK * HOT, hot_start, cold_start).astype(jnp.int32)
        start_label = jax.random.permutation(shuffle_key, start_label)
        return labels[(start_label[:, None] + offsets[None, :]) % ROUTED_EXPERTS]
    block_keys = jax.random.split(spread_keys, blocks)
    return jax.vmap(one_block)(block_keys).reshape(TOKENS, TOPK).astype(jnp.int32)


def levels(own_key, dims, cuts, smallest, high):
    def one(axis_at, parts):
        steps = jax.random.uniform(jax.random.fold_in(jax.random.fold_in(own_key, 6), axis_at), (parts,), jnp.float32, smallest / len(cuts), high / len(cuts))
        return jnp.repeat(jnp.exp(steps), dims[axis_at] // parts).reshape((-1,) + (1,) * (len(dims) - axis_at - 1))

    gain = one(*cuts[0])
    for cut in cuts[1:]:
        gain = gain * one(*cut)
    return gain


def scatter_about(own_key, shape, width, bound, cuts=(), held_as=jnp.bfloat16):
    values = width * jax.random.normal(own_key, shape, jnp.float32)
    if cuts:
        values = values * levels(own_key, shape, cuts, -0.22, 0.18)
    return jnp.clip(values, -bound, bound).astype(held_as)


def setup_inputs(seed: int = 0) -> dict:
    seeds = jax.random.split(jax.random.key(seed), 10)
    return {
        "tokens": scatter_about(seeds[0], (TOKENS, MODEL_FEATURES), 1.0, 6.0, ((0, 32),)),
        "chosen_expert_index": draw_chosen_expert_index(jax.random.fold_in(seeds[9], 71), 0),
        "router_gate_weight": jnp.clip(jnp.exp(math.log(0.5) - 2.3025851 * jax.random.uniform(seeds[2], (TOKENS, TOPK), jnp.float32) ** levels(seeds[2], (TOKENS, TOPK), ((0, 32),), -0.2, 0.2)), 0.05, 0.5),
        "output_gradient": scatter_about(seeds[3], (TOKENS, MODEL_FEATURES), 0.02, 0.15917969, ((0, 32),)),
        "gate_weight_matrix": scatter_about(seeds[4], (ROUTED_EXPERTS, MODEL_FEATURES, HIDDEN_UNITS), MODEL_FEATURES ** -0.5, 0.1875, ((0, 8),)),
        "up_weight": scatter_about(seeds[5], (ROUTED_EXPERTS, MODEL_FEATURES, HIDDEN_UNITS), MODEL_FEATURES ** -0.5, 0.1875, ((0, 8),)),
        "down_weight": scatter_about(seeds[6], (ROUTED_EXPERTS, HIDDEN_UNITS, MODEL_FEATURES), HIDDEN_UNITS ** -0.5, 0.21875, ((0, 8),)),
        "adapter_down_maps": scatter_about(seeds[7], (ROUTED_EXPERTS, ADAPTER_DEPTH, HIDDEN_UNITS), HIDDEN_UNITS ** -0.5, 0.21875, ((0, 8),)),
        "adapter_up_maps": scatter_about(seeds[8], (ROUTED_EXPERTS, ADAPTER_DEPTH, MODEL_FEATURES), ADAPTER_DEPTH ** -0.5, 1.5, ((0, 8),)),
    }


def reference(tokens, chosen_expert_index, router_gate_weight, output_gradient, gate_weight_matrix, up_weight, down_weight, adapter_down_maps, adapter_up_maps):
    total_slots = TOKENS * TOPK
    flat_ids = chosen_expert_index.reshape(total_slots).astype(jnp.int32)
    flat_gates = router_gate_weight.reshape(total_slots)
    sort_order = jnp.argsort(flat_ids, stable=True).astype(jnp.int32)
    counts = jnp.bincount(flat_ids, length=ROUTED_EXPERTS).astype(jnp.int32)
    starts = (jnp.cumsum(counts) - counts).astype(jnp.int32)
    bound_rows = (TOKENS // TOK_DEV) * CAP

    def per_expert(running, expert_number):
        position = jnp.arange(bound_rows, dtype=jnp.int32)
        is_live = position < counts[expert_number]
        slot_index = sort_order[jnp.clip(starts[expert_number] + position, 0, total_slots - 1).astype(jnp.int32)]
        token_index = (slot_index // TOPK).astype(jnp.int32)
        slot_gate = jnp.where(is_live, flat_gates[slot_index], jnp.float32(0.0))
        slot_rows = tokens[token_index]
        gate_proj = jnp.dot(slot_rows, gate_weight_matrix[expert_number], preferred_element_type=jnp.float32)
        upward = jnp.dot(slot_rows, up_weight[expert_number], preferred_element_type=jnp.float32)
        hidden_state = (jax.nn.silu(gate_proj) * upward).astype(jnp.bfloat16)
        rank_state = jnp.dot(hidden_state, adapter_down_maps[expert_number].T, preferred_element_type=jnp.float32).astype(jnp.bfloat16)
        slot_out = (jnp.dot(hidden_state, down_weight[expert_number], preferred_element_type=jnp.float32)
                    + jnp.dot(rank_state, adapter_up_maps[expert_number], preferred_element_type=jnp.float32)).astype(jnp.bfloat16)
        running = running.at[token_index].add(slot_gate[:, None] * slot_out.astype(jnp.float32))
        expert_slot_gradient = (slot_gate[:, None] * output_gradient[token_index].astype(jnp.float32)).astype(jnp.bfloat16)
        rank_gradient = jnp.dot(expert_slot_gradient, adapter_up_maps[expert_number].T, preferred_element_type=jnp.float32).astype(jnp.bfloat16)
        grad_hidden = jnp.dot(rank_gradient.T, hidden_state, preferred_element_type=jnp.float32)
        grad_model = jnp.dot(rank_state.T, expert_slot_gradient, preferred_element_type=jnp.float32)
        return running, (grad_hidden, grad_model)

    initial = jnp.zeros((TOKENS, MODEL_FEATURES), jnp.float32)
    mixed_sum, grads = lax.scan(per_expert, initial, jnp.arange(ROUTED_EXPERTS, dtype=jnp.int32))
    return mixed_sum.astype(jnp.bfloat16), grads[0].astype(jnp.bfloat16), grads[1].astype(jnp.bfloat16)
```

```python
import functools

import jax
import jax.numpy as jnp
from jax import lax
from jax.experimental import pallas as pl
from jax.experimental.pallas import tpu as pltpu
from jax.sharding import PartitionSpec as P

MESH = pl.DeviceIdType.MESH
F32 = jnp.float32
BF16 = jnp.bfloat16
CHUNKS = 2


def dot_nt(a, b):
    return lax.dot_general(a, b, (((1,), (1,)), ((), ())), preferred_element_type=F32)


def dot(a, b):
    return jnp.dot(a, b, preferred_element_type=F32)


def each(lo, hi, fn):
    def body(s, carry):
        fn(s)
        return carry

    lax.fori_loop(lo, hi, body, 0)


def line_of(n):
    return 4 if n % 4 == 0 else n


def parts_of(nd, width):
    parts = 1
    while parts * 2 <= nd and width % (parts * 2 * 128) == 0:
        parts *= 2
    return parts


def kernel(
    n,
    nd,
    tok_h,
    idx_ref,
    w_ref,
    og_ref,
    gw_h,
    uw_h,
    dw_h,
    ad_ref,
    au_h,
    mixed_ref,
    gin_ref,
    gout_ref,
    tok_all,
    gw,
    uw,
    dw,
    hid_all,
    term,
    pair_recv,
    near_recv,
    line_send,
    line_recv,
    gate_recv,
    au_all,
    lg_send,
    lg_recv,
    rk_send,
    rk_recv,
    gexp,
    gp_buf,
    gm_recv,
    ge_send,
    ge_recv,
    go_buf,
    gin_all,
    acc,
    loc_sem,
    up_s,
    down_s,
    side_s,
    tok_r,
    pair_s,
    pair_r,
    near_s,
    near_r,
    line_s,
    line_r,
    gate_s,
    gate_r,
    au_s,
    au_r,
    am_s,
    am_r,
    lg_s,
    lg_r,
    rk_s,
    rk_r,
    gm_s,
    gm_r,
    ge_s,
    ge_r,
    go_s,
    go_r,
    gin_s,
    gin_r,
):
    me = lax.axis_index("expert")
    rep = lax.axis_index("dp")
    line = line_of(n)
    side = n // line
    at_line = me // side
    at_side = lax.rem(me, side)
    rows = tok_all.shape[1]
    rank = ad_ref.shape[1]
    width = tok_all.shape[2]
    hidden = ad_ref.shape[2]
    parts = parts_of(nd, width)
    part = width // parts
    cr = rows // CHUNKS
    owner = rep < parts

    def peer(s):
        return lax.rem(me + s, n)

    def mate(s):
        return lax.rem(rep + s, nd)

    def other(s):
        return lax.rem(at_side + s, side)

    def to_expert(src, dst, s_sem, r_sem, p):
        return pltpu.make_async_remote_copy(
            src_ref=src,
            dst_ref=dst,
            send_sem=s_sem,
            recv_sem=r_sem,
            device_id={"expert": p},
            device_id_type=MESH,
        )

    def to_mate(src, dst, s_sem, r_sem, p):
        return pltpu.make_async_remote_copy(
            src_ref=src,
            dst_ref=dst,
            send_sem=s_sem,
            recv_sem=r_sem,
            device_id={"dp": p},
            device_id_type=MESH,
        )

    def on_line(z):
        return (z >= 0) & (z < line)

    def chunk(c):
        return pl.ds(pl.multiple_of(c * cr, cr), cr)

    def cols(p):
        return pl.ds(pl.multiple_of(p * part, part), part)

    loads = [
        pltpu.make_async_copy(tok_h, tok_all.at[me], loc_sem.at[0]),
        pltpu.make_async_copy(gw_h.at[0], gw, loc_sem.at[1]),
        pltpu.make_async_copy(uw_h.at[0], uw, loc_sem.at[2]),
        pltpu.make_async_copy(dw_h.at[0], dw.at[pl.ds(0, hidden)], loc_sem.at[3]),
        pltpu.make_async_copy(au_h.at[0], dw.at[pl.ds(hidden, rank)], loc_sem.at[4]),
    ]
    for load in loads:
        load.start()

    def load_map():
        return pltpu.make_async_copy(
            au_h.at[0, :, cols(rep)], au_all.at[me, :, cols(rep)], loc_sem.at[5]
        )

    @pl.when(owner)
    def _():
        load_map().start()

    barrier = pltpu.get_barrier_semaphore()
    each(
        1,
        n,
        lambda s: pl.semaphore_signal(
            barrier, inc=1, device_id={"expert": peer(s)}, device_id_type=MESH
        ),
    )
    each(
        1,
        nd,
        lambda s: pl.semaphore_signal(
            barrier, inc=1, device_id={"dp": mate(s)}, device_id_type=MESH
        ),
    )

    eye = lax.broadcasted_iota(jnp.int32, (rows, rows), 0) == lax.broadcasted_iota(
        jnp.int32, (rows, rows), 1
    )

    def spread_gates(e):
        row = jnp.sum(jnp.where(idx_ref[...] == e, w_ref[...], 0.0), axis=0, keepdims=True)
        gexp[e] = jnp.broadcast_to(row, (rank, rows))

    each(0, n, spread_gates)
    gate_recv[me] = gexp[me, 0:8]

    def up_copy(z, c):
        k = z * side + at_side
        p = (at_line + 1) * side + at_side
        ref = tok_all.at[k, chunk(c)]
        return to_expert(ref, ref, up_s.at[z, c], tok_r.at[k, c], p)

    def down_copy(z, c):
        k = z * side + at_side
        p = (at_line - 1) * side + at_side
        ref = tok_all.at[k, chunk(c)]
        return to_expert(ref, ref, down_s.at[z, c], tok_r.at[k, c], p)

    def side_copy(z, s, c):
        k = z * side + at_side
        x = other(s)
        p = at_line * side + x
        ref = tok_all.at[k, chunk(c)]
        return to_expert(ref, ref, side_s.at[z * side + x, c], tok_r.at[k, c], p)

    def gate_copy(s):
        p = peer(s)
        return to_expert(
            gexp.at[p, pl.ds(0, 8)], gate_recv.at[me], gate_s.at[p], gate_r.at[me], p
        )

    def au_copy(s):
        p = peer(s)
        ref = au_all.at[me, :, cols(rep)]
        return to_expert(ref, ref, au_s.at[p], au_r.at[me], p)

    def am_copy(s):
        p = mate(s)
        ref = au_all.at[:, :, cols(rep)]
        return to_mate(ref, ref, am_s.at[p], am_r.at[rep], p)

    def pair_copy(z, x, c):
        k = z * side + x
        p = at_line * side + x
        mine = z * side + at_side
        return to_expert(
            term.at[k, chunk(c)], pair_recv.at[mine, chunk(c)], pair_s.at[k, c],
            pair_r.at[mine, c], p,
        )

    def near_copy(z, x):
        b = jnp.where(z > at_line, 0, 1)
        p = z * side + at_side
        return to_expert(
            term.at[z * side + x], near_recv.at[b, x], near_s.at[b, x], near_r.at[b, x], p
        )

    def line_copy(z, c):
        p = z * side + at_side
        return to_expert(
            line_send.at[z, chunk(c)], line_recv.at[at_line, chunk(c)], line_s.at[z, c],
            line_r.at[at_line, c], p,
        )

    def lg_copy(s):
        p = peer(s)
        return to_expert(lg_send.at[p], lg_recv.at[me], lg_s.at[p], lg_r.at[me], p)

    def rk_copy(p):
        return to_expert(rk_send.at[p], rk_recv.at[me], rk_s.at[p], rk_r.at[me], p)

    def gm_copy(s):
        p = mate(s)
        return to_mate(gp_buf.at[:, cols(p)], gm_recv.at[rep], gm_s.at[p], gm_r.at[rep], p)

    def ge_copy(s):
        p = peer(s)
        return to_expert(ge_send.at[p], ge_recv.at[me], ge_s.at[p], ge_r.at[me], p)

    def go_copy(s):
        p = mate(s)
        ref = go_buf.at[:, cols(rep)]
        return to_mate(ref, ref, go_s.at[p], go_r.at[rep], p)

    def gin_copy(s):
        p = mate(s)
        return to_mate(gin_all.at[rep], gin_all.at[rep], gin_s.at[p], gin_r.at[rep], p)

    def arrived(ref, sem):
        to_expert(ref, ref, sem, sem, me).wait_recv()

    def arrived_tok(k, c):
        arrived(tok_all.at[k, chunk(c)], tok_r.at[k, c])

    def spread(z, c, go_up, go_down):
        each(1, side, lambda s: side_copy(z, s, c).start())

        @pl.when(go_up & (at_line + 1 < line))
        def _():
            up_copy(z, c).start()

        @pl.when(go_down & (at_line >= 1))
        def _():
            down_copy(z, c).start()

    loads[0].wait()
    pl.semaphore_wait(barrier, n - 1 + nd - 1)

    each(1, n, lambda s: gate_copy(s).start())
    each(0, CHUNKS, lambda c: spread(at_line, c, True, True))
    for load in loads[1:]:
        load.wait()

    @pl.when(owner)
    def _():
        load_map().wait()
        each(1, n, lambda s: au_copy(s).start())

    def share_maps():
        @pl.when(owner)
        def _():
            def arrived_au(s):
                p = peer(s)
                arrived(au_all.at[p, :, cols(rep)], au_r.at[p])

            each(1, n, arrived_au)
            each(1, nd, lambda s: am_copy(s).start())

    def low_grads():
        def arrived_am(s):
            p = mate(s)

            @pl.when(p < parts)
            def _():
                arrived(au_all.at[:, :, cols(p)], am_r.at[p])

        each(1, nd, arrived_am)
        low_grad = dot_nt(au_all[...].reshape(n * rank, width), og_ref[...])
        low_grad = low_grad * gexp[...].reshape(n * rank, rows)
        lg_send[...] = low_grad.astype(BF16).reshape(n, rank, rows)
        lg_recv[me] = lg_send[me]
        each(1, n, lambda s: lg_copy(s).start())

    def relay(k):
        def piece(c):
            for sign in (-1, 1):
                z = at_line + sign * k

                @pl.when((k >= 1) & on_line(z))
                def _():
                    arrived_tok(z * side + at_side, c)
                    spread(z, c, sign < 0, sign > 0)

        each(0, CHUNKS, piece)

    def expert_block(src):
        x = tok_all[src]
        g = dot_nt(x, gw[...])
        u = dot_nt(x, uw[...])
        h = (g / (1.0 + jnp.exp(-g)) * u).astype(BF16)
        low = dot_nt(h, ad_ref[0])
        hid_all[src, :, 0:hidden] = h
        hid_all[src, :, hidden : hidden + rank] = low.astype(BF16)
        out = dot(hid_all[src], dw[...]).astype(BF16)
        return low.T.astype(BF16), out

    def work(k, j):
        s = j // 2
        sign = 1 - 2 * lax.rem(j, 2)
        far = k - jnp.minimum(s, 1)
        z = at_line + sign * far
        x = other(s)
        src = z * side + x

        @pl.when(on_line(z) & (far >= 0) & ((far > 0) | (sign > 0)))
        def _():
            @pl.when(s > 0)
            def _():
                each(0, CHUNKS, lambda c: arrived_tok(src, c))

            @pl.when(src != me)
            def _():
                arrived(gate_recv.at[src], gate_r.at[src])

            low_t, out = expert_block(src)
            row = gate_recv[src, 0:1]
            column = jnp.sum(jnp.where(eye, row, 0.0), axis=1, keepdims=True)
            term[src] = (out.astype(F32) * column).astype(BF16)

            @pl.when(src == me)
            def _():
                rk_recv[me] = low_t

            @pl.when(src != me)
            def _():
                rk_send[src] = low_t
                rk_copy(src).start()

            @pl.when((s > 0) & (far == 1))
            def _():
                near_copy(z, x).start()

            @pl.when((s > 0) & (far >= 2))
            def _():
                each(0, CHUNKS, lambda c: pair_copy(z, x, c).start())

    def near_own():
        for sign in (-1, 1):
            z = at_line + sign

            @pl.when(on_line(z))
            def _():
                near_copy(z, at_side).start()

    def step(k):
        relay(k)
        pl.when(k == 2)(near_own)
        each(0, 2 * side, lambda j: work(k, j))
        pl.when(k == 1)(share_maps)
        pl.when(k == 2)(low_grads)

    each(0, line + 1, step)

    def pairs(k):
        for sign in (-1, 1):
            z = at_line + sign * k

            @pl.when(on_line(z))
            def _():
                def piece(c):
                    def wait_pair(s):
                        src = z * side + other(s)
                        arrived(pair_recv.at[src, chunk(c)], pair_r.at[src, c])

                    each(1, side, wait_pair)

                    def add(s, total):
                        return total + pair_recv[z * side + other(s), chunk(c)].astype(F32)

                    total = lax.fori_loop(
                        1, side, add, term[z * side + at_side, chunk(c)].astype(F32)
                    )
                    line_send[z, chunk(c)] = total.astype(BF16)
                    line_copy(z, c).start()

                each(0, CHUNKS, piece)

    def near_sum(x, total_ref):
        total_ref[...] = term[at_line * side + x].astype(F32)

        @pl.when(at_line >= 1)
        def _():
            arrived(near_recv.at[0, x], near_r.at[0, x])
            total_ref[...] += near_recv[0, x].astype(F32)

        @pl.when(at_line + 1 < line)
        def _():
            arrived(near_recv.at[1, x], near_r.at[1, x])
            total_ref[...] += near_recv[1, x].astype(F32)

    def merge(s):
        x = other(s)
        near_sum(x, acc)
        term[at_line * side + x] = acc[...].astype(BF16)
        each(0, CHUNKS, lambda c: pair_copy(at_line, x, c).start())

    def in_grads():
        def arrived_lg(s):
            p = peer(s)
            arrived(lg_recv.at[p], lg_r.at[p])

        each(1, n, arrived_lg)

        def add_gin(src, total):
            return total + dot(lg_recv[src], hid_all[src])

        gin_all[rep] = lax.fori_loop(0, n, add_gin, jnp.zeros(gin_all.shape[1:], F32))
        each(1, nd, lambda s: gin_copy(s).start())

    def out_grads():
        def arrived_rk(s):
            p = peer(s)
            arrived(rk_recv.at[p], rk_r.at[p])

        each(1, n, arrived_rk)
        low_w = (rk_recv[...].astype(F32) * gexp[...]).astype(BF16).reshape(n * rank, rows)
        gp_buf[...] = dot(low_w, og_ref[...]).astype(BF16)

        def send(s):
            @pl.when(mate(s) < parts)
            def _():
                gm_copy(s).start()

        each(1, nd, send)

    def mate_sum():
        @pl.when(owner)
        def _():
            def add(s, total):
                p = mate(s)
                arrived(gm_recv.at[p], gm_r.at[p])
                return total + gm_recv[p].astype(F32)

            total = lax.fori_loop(1, nd, add, gp_buf[:, cols(rep)].astype(F32))
            ge_send[...] = total.astype(BF16).reshape(n, rank, part)
            each(1, n, lambda s: ge_copy(s).start())

    def expert_sum():
        @pl.when(owner)
        def _():
            def add(s, total):
                p = peer(s)
                arrived(ge_recv.at[p], ge_r.at[p])
                return total + ge_recv[p].astype(F32)

            total = lax.fori_loop(1, n, add, ge_send[me].astype(F32))
            go_buf[:, cols(rep)] = total.astype(BF16)
            each(1, nd, lambda s: go_copy(s).start())

    in_grads()
    pairs(2)
    out_grads()
    each(1, side, merge)
    for k in range(3, line):
        pairs(k)
    mate_sum()

    near_sum(at_side, acc)

    def add_merged(s):
        src = at_line * side + other(s)
        each(0, CHUNKS, lambda c: arrived(pair_recv.at[src, chunk(c)], pair_r.at[src, c]))
        acc[...] += pair_recv[src].astype(F32)

    each(1, side, add_merged)
    expert_sum()

    for k in range(2, line):
        for sign in (-1, 1):
            z = at_line + sign * k

            @pl.when(on_line(z))
            def _():
                each(
                    0, CHUNKS, lambda c: arrived(line_recv.at[z, chunk(c)], line_r.at[z, c])
                )
                acc[...] += line_recv[z].astype(F32)

    mixed_ref[...] = acc[...].astype(BF16)

    def arrived_gin(s):
        p = mate(s)
        arrived(gin_all.at[p], gin_r.at[p])

    each(1, nd, arrived_gin)
    gin_ref[0] = jnp.sum(gin_all[...], axis=0)[:, 0:hidden].astype(BF16)

    def arrived_go(s):
        p = mate(s)

        @pl.when(p < parts)
        def _():
            arrived(go_buf.at[:, cols(p)], go_r.at[p])

    each(1, nd, arrived_go)
    gout_ref[0] = go_buf[...]

    def drain(s):
        gate_copy(s).wait_send()
        lg_copy(s).wait_send()
        rk_copy(peer(s)).wait_send()

        @pl.when(owner)
        def _():
            au_copy(s).wait_send()
            ge_copy(s).wait_send()

    each(1, n, drain)

    def drain_line(z):
        def piece(c):
            @pl.when((z <= at_line) & (at_line + 1 < line))
            def _():
                up_copy(z, c).wait_send()

            @pl.when((z >= at_line) & (at_line >= 1))
            def _():
                down_copy(z, c).wait_send()

            each(1, side, lambda s: side_copy(z, s, c).wait_send())

            @pl.when((z == at_line) | (z - at_line >= 2) | (at_line - z >= 2))
            def _():
                each(1, side, lambda s: pair_copy(z, other(s), c).wait_send())

            @pl.when((z - at_line >= 2) | (at_line - z >= 2))
            def _():
                line_copy(z, c).wait_send()

        each(0, CHUNKS, piece)

        @pl.when((z - at_line == 1) | (at_line - z == 1))
        def _():
            each(0, side, lambda x: near_copy(z, x).wait_send())

    each(0, line, drain_line)

    def drain_mates(s):
        gin_copy(s).wait_send()

        @pl.when(mate(s) < parts)
        def _():
            gm_copy(s).wait_send()

        @pl.when(owner)
        def _():
            am_copy(s).wait_send()
            go_copy(s).wait_send()

    each(1, nd, drain_mates)


def hand_over(a_ref, b_ref, c_ref, x_ref, y_ref, z_ref):
    x_ref[...] = a_ref[...]
    y_ref[...] = b_ref[...]
    z_ref[...] = c_ref[...]


def shards(
    n,
    nd,
    tokens,
    chosen_expert_index,
    router_gate_weight,
    output_gradient,
    gate_weight_matrix,
    up_weight,
    down_weight,
    adapter_down_maps,
    adapter_up_maps,
):
    rows, width = tokens.shape
    rank, hidden = adapter_down_maps.shape[1:]
    line = line_of(n)
    side = n // line
    parts = parts_of(nd, width)
    part = width // parts
    vmem = pl.BlockSpec(memory_space=pltpu.VMEM)
    anywhere = pl.BlockSpec(memory_space=pl.ANY)
    dma = pltpu.SemaphoreType.DMA
    results = pl.pallas_call(
        functools.partial(kernel, n, nd),
        out_shape=(
            jax.ShapeDtypeStruct((rows, width), BF16),
            jax.ShapeDtypeStruct((1, rank, hidden), BF16),
            jax.ShapeDtypeStruct((1, rank, width), BF16),
        ),
        in_specs=[anywhere, vmem, vmem, vmem, anywhere, anywhere, anywhere, vmem, anywhere],
        out_specs=(vmem, vmem, vmem),
        scratch_shapes=[
            pltpu.VMEM((n, rows, width), BF16),
            pltpu.VMEM((hidden, width), BF16),
            pltpu.VMEM((hidden, width), BF16),
            pltpu.VMEM((hidden + rank, width), BF16),
            pltpu.VMEM((n, rows, hidden + rank), BF16),
            pltpu.VMEM((n, rows, width), BF16),
            pltpu.VMEM((n, rows, width), BF16),
            pltpu.VMEM((2, side, rows, width), BF16),
            pltpu.VMEM((line, rows, width), BF16),
            pltpu.VMEM((line, rows, width), BF16),
            pltpu.VMEM((n, 8, rows), F32),
            pltpu.VMEM((n, rank, width), BF16),
            pltpu.VMEM((n, rank, rows), BF16),
            pltpu.VMEM((n, rank, rows), BF16),
            pltpu.VMEM((n, rank, rows), BF16),
            pltpu.VMEM((n, rank, rows), BF16),
            pltpu.VMEM((n, rank, rows), F32),
            pltpu.VMEM((n * rank, width), BF16),
            pltpu.VMEM((nd, n * rank, part), BF16),
            pltpu.VMEM((n, rank, part), BF16),
            pltpu.VMEM((n, rank, part), BF16),
            pltpu.VMEM((rank, width), BF16),
            pltpu.VMEM((nd, rank, hidden + rank), F32),
            pltpu.VMEM((rows, width), F32),
            dma((6,)),
        ]
        + [dma((line, CHUNKS))] * 2
        + [dma((n, CHUNKS))] * 4
        + [dma((2, side))] * 2
        + [dma((line, CHUNKS))] * 2
        + [dma((n,))] * 4
        + [dma((nd,))] * 2
        + [dma((n,))] * 4
        + [dma((nd,))] * 2
        + [dma((n,))] * 2
        + [dma((nd,))] * 4,
        compiler_params=pltpu.CompilerParams(
            collective_id=0, has_side_effects=True, vmem_limit_bytes=60 * 1024 * 1024
        ),
    )(
        tokens,
        chosen_expert_index.T,
        router_gate_weight.T,
        output_gradient,
        jnp.swapaxes(gate_weight_matrix, 1, 2),
        jnp.swapaxes(up_weight, 1, 2),
        down_weight,
        adapter_down_maps,
        adapter_up_maps,
    )
    return pl.pallas_call(
        hand_over,
        out_shape=tuple(jax.ShapeDtypeStruct(r.shape, r.dtype) for r in results),
        in_specs=[vmem] * 3,
        out_specs=(vmem,) * 3,
    )(*results)


def solution(mesh):
    return jax.shard_map(
        functools.partial(shards, mesh.shape["expert"], mesh.shape["dp"]),
        mesh=mesh,
        in_specs=(
            P(("dp", "expert"), None),
            P(("dp", "expert"), None),
            P(("dp", "expert"), None),
            P(("dp", "expert"), None),
            P("expert", None, None),
            P("expert", None, None),
            P("expert", None, None),
            P("expert", None, None),
            P("expert", None, None),
        ),
        out_specs=(P(("dp", "expert"), None), P("expert", None, None), P("expert", None, None)),
        check_vma=False,
    )
```

```python
import functools

import jax
import jax.numpy as jnp
from jax import lax
from jax.experimental import pallas as pl
from jax.experimental.pallas import tpu as pltpu
from jax.sharding import PartitionSpec as P

MESH = pl.DeviceIdType.MESH
F32 = jnp.float32
BF16 = jnp.bfloat16
CHUNKS = 2


def dot_nt(a, b):
    return lax.dot_general(a, b, (((1,), (1,)), ((), ())), preferred_element_type=F32)


def dot(a, b):
    return jnp.dot(a, b, preferred_element_type=F32)


def each(lo, hi, fn):
    def body(s, carry):
        fn(s)
        return carry

    lax.fori_loop(lo, hi, body, 0)


def line_of(n):
    assert n % 4 == 0
    return 4


OUTER = ((0, 0), (1, 0), (0, 1), (2, 0), (1, 1), (2, 1), (3, 0), (3, 1))
INNER = ((0, 0), (1, 0), (-1, 0), (0, 1), (1, 1), (-1, 1), (2, 1), (2, 0))
RELAYS = {1: ((1, 0), (1, 1)), 2: ((2, 0),), 3: ((2, 1),), 5: ((3, 0), (3, 1))}


def parts_of(nd, width):
    parts = 1
    while parts * 2 <= nd and width % (parts * 2 * 128) == 0:
        parts *= 2
    return parts


def kernel(
    n,
    nd,
    tok_h,
    idx_ref,
    w_ref,
    og_ref,
    gw_h,
    uw_h,
    dw_h,
    ad_ref,
    au_h,
    mixed_ref,
    gin_ref,
    gout_ref,
    tok_all,
    gw,
    uw,
    dw,
    hid_all,
    term,
    pair_recv,
    near_recv,
    line_send,
    line_recv,
    gate_recv,
    au_all,
    lg_send,
    lg_recv,
    rk_send,
    rk_recv,
    gexp,
    gp_buf,
    gm_recv,
    ge_send,
    ge_recv,
    go_buf,
    gin_all,
    acc,
    loc_sem,
    up_s,
    down_s,
    side_s,
    onward_s,
    tok_r,
    pair_s,
    pair_r,
    near_s,
    near_r,
    line_s,
    line_r,
    gate_s,
    gate_r,
    au_s,
    au_r,
    am_s,
    am_r,
    lg_s,
    lg_r,
    rk_s,
    rk_r,
    gm_s,
    gm_r,
    ge_s,
    ge_r,
    go_s,
    go_r,
    gin_s,
    gin_r,
):
    me = lax.axis_index("expert")
    rep = lax.axis_index("dp")
    line = line_of(n)
    side = n // line
    at_line = me // side
    at_side = lax.rem(me, side)
    rows = tok_all.shape[1]
    rank = ad_ref.shape[1]
    width = tok_all.shape[2]
    hidden = ad_ref.shape[2]
    parts = parts_of(nd, width)
    part = width // parts
    cr = rows // CHUNKS
    owner = rep < parts
    front = jnp.where(2 * at_line < line, 1, -1)
    outer = (at_line == 0) | (at_line == line - 1)

    def peer(s):
        return lax.rem(me + s, n)

    def mate(s):
        return lax.rem(rep + s, nd)

    def other(s):
        return lax.rem(at_side + s, side)

    def to_expert(src, dst, s_sem, r_sem, p):
        return pltpu.make_async_remote_copy(
            src_ref=src,
            dst_ref=dst,
            send_sem=s_sem,
            recv_sem=r_sem,
            device_id={"expert": p},
            device_id_type=MESH,
        )

    def to_mate(src, dst, s_sem, r_sem, p):
        return pltpu.make_async_remote_copy(
            src_ref=src,
            dst_ref=dst,
            send_sem=s_sem,
            recv_sem=r_sem,
            device_id={"dp": p},
            device_id_type=MESH,
        )

    def on_line(z):
        return (z >= 0) & (z < line)

    def chunk(c):
        return pl.ds(pl.multiple_of(c * cr, cr), cr)

    def cols(p):
        return pl.ds(pl.multiple_of(p * part, part), part)

    loads = [
        pltpu.make_async_copy(tok_h, tok_all.at[me], loc_sem.at[0]),
        pltpu.make_async_copy(gw_h.at[0], gw, loc_sem.at[1]),
        pltpu.make_async_copy(uw_h.at[0], uw, loc_sem.at[2]),
        pltpu.make_async_copy(dw_h.at[0], dw.at[pl.ds(0, hidden)], loc_sem.at[3]),
        pltpu.make_async_copy(au_h.at[0], dw.at[pl.ds(hidden, rank)], loc_sem.at[4]),
    ]
    for load in loads:
        load.start()

    def load_map():
        return pltpu.make_async_copy(
            au_h.at[0, :, cols(rep)], au_all.at[me, :, cols(rep)], loc_sem.at[5]
        )

    @pl.when(owner)
    def _():
        load_map().start()

    barrier = pltpu.get_barrier_semaphore()
    each(
        1,
        n,
        lambda s: pl.semaphore_signal(
            barrier, inc=1, device_id={"expert": peer(s)}, device_id_type=MESH
        ),
    )
    each(
        1,
        nd,
        lambda s: pl.semaphore_signal(
            barrier, inc=1, device_id={"dp": mate(s)}, device_id_type=MESH
        ),
    )

    eye = lax.broadcasted_iota(jnp.int32, (rows, rows), 0) == lax.broadcasted_iota(
        jnp.int32, (rows, rows), 1
    )

    def spread_gates(e):
        row = jnp.sum(jnp.where(idx_ref[...] == e, w_ref[...], 0.0), axis=0, keepdims=True)
        gexp[e] = jnp.broadcast_to(row, (rank, rows))

    each(0, n, spread_gates)
    gate_recv[me] = gexp[me, 0:1]

    def up_copy(z, c):
        k = z * side + at_side
        p = (at_line + 1) * side + at_side
        ref = tok_all.at[k, chunk(c)]
        return to_expert(ref, ref, up_s.at[z, c], tok_r.at[k, c], p)

    def down_copy(z, c):
        k = z * side + at_side
        p = (at_line - 1) * side + at_side
        ref = tok_all.at[k, chunk(c)]
        return to_expert(ref, ref, down_s.at[z, c], tok_r.at[k, c], p)

    def side_copy(z, s, c):
        k = z * side + at_side
        x = other(s)
        p = at_line * side + x
        ref = tok_all.at[k, chunk(c)]
        return to_expert(ref, ref, side_s.at[z * side + x, c], tok_r.at[k, c], p)

    def onward_copy(s, c):
        x = other(s)
        ref = tok_all.at[at_line * side + x, chunk(c)]
        p = (at_line + front) * side + at_side
        return to_expert(ref, ref, onward_s.at[x, c], tok_r.at[at_line * side + x, c], p)

    def gate_copy(s):
        p = peer(s)
        return to_expert(
            gexp.at[p, pl.ds(0, 1)], gate_recv.at[me], gate_s.at[p], gate_r.at[me], p
        )

    def au_copy(s):
        p = peer(s)
        ref = au_all.at[me, :, cols(rep)]
        return to_expert(ref, ref, au_s.at[p], au_r.at[me], p)

    def am_copy(s):
        p = mate(s)
        ref = au_all.at[:, :, cols(rep)]
        return to_mate(ref, ref, am_s.at[p], am_r.at[rep], p)

    def pair_copy(z, x, c):
        k = z * side + x
        p = at_line * side + x
        mine = z * side + at_side
        return to_expert(
            term.at[k, chunk(c)], pair_recv.at[mine, chunk(c)], pair_s.at[k, c],
            pair_r.at[mine, c], p,
        )

    def near_copy(z, x):
        b = jnp.where(z > at_line, 0, 1)
        p = z * side + at_side
        return to_expert(
            term.at[z * side + x], near_recv.at[b, x], near_s.at[b, x], near_r.at[b, x], p
        )

    def line_copy(z, c):
        p = z * side + at_side
        return to_expert(
            line_send.at[z, chunk(c)], line_recv.at[at_line, chunk(c)], line_s.at[z, c],
            line_r.at[at_line, c], p,
        )

    def lg_copy(s):
        p = peer(s)
        return to_expert(lg_send.at[p], lg_recv.at[me], lg_s.at[p], lg_r.at[me], p)

    def rk_copy(p):
        return to_expert(rk_send.at[p], rk_recv.at[me], rk_s.at[p], rk_r.at[me], p)

    def gm_copy(s):
        p = mate(s)
        return to_mate(gp_buf.at[:, cols(p)], gm_recv.at[rep], gm_s.at[p], gm_r.at[rep], p)

    def ge_copy(s):
        p = peer(s)
        return to_expert(ge_send.at[p], ge_recv.at[me], ge_s.at[p], ge_r.at[me], p)

    def go_copy(s):
        p = mate(s)
        ref = go_buf.at[:, cols(rep)]
        return to_mate(ref, ref, go_s.at[p], go_r.at[rep], p)

    def gin_copy(s):
        p = mate(s)
        return to_mate(gin_all.at[rep], gin_all.at[rep], gin_s.at[p], gin_r.at[rep], p)

    def arrived(ref, sem):
        to_expert(ref, ref, sem, sem, me).wait_recv()

    def arrived_tok(k, c):
        arrived(tok_all.at[k, chunk(c)], tok_r.at[k, c])

    def crosses(z):
        return outer | (z != at_line - front)

    def spread(z, c, go_up, go_down):
        @pl.when(crosses(z))
        def _():
            each(1, side, lambda s: side_copy(z, s, c).start())

        @pl.when(go_up & (at_line + 1 < line))
        def _():
            up_copy(z, c).start()

        @pl.when(go_down & (at_line >= 1))
        def _():
            down_copy(z, c).start()

    loads[0].wait()
    pl.semaphore_wait(barrier, n - 1 + nd - 1)

    each(1, n, lambda s: gate_copy(s).start())
    each(0, CHUNKS, lambda c: spread(at_line, c, True, True))
    for load in loads[1:]:
        load.wait()

    def send_maps():
        @pl.when(owner)
        def _():
            load_map().wait()
            each(1, n, lambda s: au_copy(s).start())

    def share_maps():
        @pl.when(owner)
        def _():
            def arrived_au(s):
                p = peer(s)
                arrived(au_all.at[p, :, cols(rep)], au_r.at[p])

            each(1, n, arrived_au)
            each(1, nd, lambda s: am_copy(s).start())

    def low_grads():
        def arrived_am(s):
            p = mate(s)

            @pl.when(p < parts)
            def _():
                arrived(au_all.at[:, :, cols(p)], am_r.at[p])

        each(1, nd, arrived_am)
        low_grad = dot_nt(au_all[...].reshape(n * rank, width), og_ref[...])
        low_grad = low_grad * gexp[...].reshape(n * rank, rows)
        lg_send[...] = low_grad.astype(BF16).reshape(n, rank, rows)
        lg_recv[me] = lg_send[me]
        each(1, n, lambda s: lg_copy(s).start())

    def relay(k, c):
        for sign in (-1, 1):
            z = at_line + sign * k

            @pl.when((k >= 1) & on_line(z))
            def _():
                arrived_tok(z * side + at_side, c)
                spread(z, c, sign < 0, sign > 0)

        @pl.when((k == 1) & outer)
        def _():
            def onward(s):
                arrived_tok(at_line * side + other(s), c)
                onward_copy(s, c).start()

            each(1, side, onward)

    def expert_block(src):
        x = tok_all[src]
        g = dot_nt(x, gw[...])
        u = dot_nt(x, uw[...])
        h = (g / (1.0 + jnp.exp(-g)) * u).astype(BF16)
        low = dot_nt(h, ad_ref[0])
        hid_all[src, :, 0:hidden] = h
        hid_all[src, :, hidden : hidden + rank] = low.astype(BF16)
        out = dot(hid_all[src], dw[...]).astype(BF16)
        return low.T.astype(BF16), out

    def work(dist, s):
        z = at_line + front * dist
        x = other(s)
        src = z * side + x

        def run():
            @pl.when((s > 0) & ((dist != 0) | ~outer))
            def _():
                each(0, CHUNKS, lambda c: arrived_tok(src, c))

            @pl.when(src != me)
            def _():
                arrived(gate_recv.at[src], gate_r.at[src])

            low_t, out = expert_block(src)
            row = gate_recv[src, 0:1]
            column = jnp.sum(jnp.where(eye, row, 0.0), axis=1, keepdims=True)
            term[src] = (out.astype(F32) * column).astype(BF16)

            @pl.when(src == me)
            def _():
                rk_recv[me] = low_t

            @pl.when(src != me)
            def _():
                rk_send[src] = low_t
                rk_copy(src).start()

            @pl.when((s > 0) & ((dist == 1) | (dist == -1)))
            def _():
                near_copy(z, x).start()

            @pl.when((s > 0) & (dist >= 2))
            def _():
                each(0, CHUNKS, lambda c: pair_copy(z, x, c).start())

        run()

    def near_own(z):
        @pl.when(on_line(z))
        def _():
            near_copy(z, at_side).start()

    def pick(i, values):
        total = 0
        for j, value in enumerate(values):
            total = total + value * (i == j).astype(jnp.int32)
        return total

    def step(i):
        for at, pieces in RELAYS.items():

            @pl.when(i == at)
            def _():
                for k, c in pieces:
                    relay(k, c)

        pl.when(i == 3)(lambda: near_own(at_line + front))
        pl.when(i == 5)(lambda: near_own(at_line - front))
        inner = 1 - outer.astype(jnp.int32)
        dist = pick(i, [d for d, _ in OUTER]) * (1 - inner) + pick(i, [d for d, _ in INNER]) * inner
        cross = pick(i, [c for _, c in OUTER]) * (1 - inner) + pick(i, [c for _, c in INNER]) * inner
        each(cross, 1 + cross * (side - 1), lambda s: work(dist, s))
        pl.when(i == 1)(send_maps)
        pl.when(i == 4)(share_maps)
        pl.when(i == 6)(low_grads)

    each(0, len(OUTER), step)

    def pairs(k, c):
        for sign in (-1, 1):
            z = at_line + sign * k

            @pl.when(on_line(z))
            def _():
                def piece():
                    def wait_pair(s):
                        src = z * side + other(s)
                        arrived(pair_recv.at[src, chunk(c)], pair_r.at[src, c])

                    each(1, side, wait_pair)

                    def add(s, total):
                        return total + pair_recv[z * side + other(s), chunk(c)].astype(F32)

                    total = lax.fori_loop(
                        1, side, add, term[z * side + at_side, chunk(c)].astype(F32)
                    )
                    line_send[z, chunk(c)] = total.astype(BF16)
                    line_copy(z, c).start()

                piece()

    def near_sum(x, total_ref):
        total_ref[...] = term[at_line * side + x].astype(F32)

        @pl.when(at_line >= 1)
        def _():
            arrived(near_recv.at[0, x], near_r.at[0, x])
            total_ref[...] += near_recv[0, x].astype(F32)

        @pl.when(at_line + 1 < line)
        def _():
            arrived(near_recv.at[1, x], near_r.at[1, x])
            total_ref[...] += near_recv[1, x].astype(F32)

    def merge(s):
        x = other(s)
        near_sum(x, acc)
        term[at_line * side + x] = acc[...].astype(BF16)

    def send_merged(c):
        each(1, side, lambda s: pair_copy(at_line, other(s), c).start())

    def in_grads():
        def arrived_lg(s):
            p = peer(s)
            arrived(lg_recv.at[p], lg_r.at[p])

        each(1, n, arrived_lg)

        def add_gin(src, total):
            return total + dot(lg_recv[src], hid_all[src])

        gin_all[rep] = lax.fori_loop(0, n, add_gin, jnp.zeros(gin_all.shape[1:], F32))
        each(1, nd, lambda s: gin_copy(s).start())

    def out_grads():
        def arrived_rk(s):
            p = peer(s)
            arrived(rk_recv.at[p], rk_r.at[p])

        each(1, n, arrived_rk)
        low_w = (rk_recv[...].astype(F32) * gexp[...]).astype(BF16).reshape(n * rank, rows)
        gp_buf[...] = dot(low_w, og_ref[...]).astype(BF16)

        def send(s):
            @pl.when(mate(s) < parts)
            def _():
                gm_copy(s).start()

        each(1, nd, send)

    def mate_sum():
        @pl.when(owner)
        def _():
            def add(s, total):
                p = mate(s)
                arrived(gm_recv.at[p], gm_r.at[p])
                return total + gm_recv[p].astype(F32)

            total = lax.fori_loop(1, nd, add, gp_buf[:, cols(rep)].astype(F32))
            ge_send[...] = total.astype(BF16).reshape(n, rank, part)
            each(1, n, lambda s: ge_copy(s).start())

    def expert_sum():
        @pl.when(owner)
        def _():
            def add(s, total):
                p = peer(s)
                arrived(ge_recv.at[p], ge_r.at[p])
                return total + ge_recv[p].astype(F32)

            total = lax.fori_loop(1, n, add, ge_send[me].astype(F32))
            go_buf[:, cols(rep)] = total.astype(BF16)
            each(1, nd, lambda s: go_copy(s).start())

    for c in range(CHUNKS):
        pairs(2, c)
    each(1, side, merge)
    pl.when(~outer)(lambda: each(0, CHUNKS, send_merged))
    out_grads()
    for c in range(CHUNKS):
        for k in range(3, line):
            pairs(k, c)
        pl.when(outer)(lambda c=c: send_merged(c))
    mate_sum()
    in_grads()
    near_sum(at_side, acc)
    expert_sum()

    def add_merged(s):
        src = at_line * side + other(s)
        each(0, CHUNKS, lambda c: arrived(pair_recv.at[src, chunk(c)], pair_r.at[src, c]))
        acc[...] += pair_recv[src].astype(F32)

    each(1, side, add_merged)

    for k in range(2, line):
        for sign in (-1, 1):
            z = at_line + sign * k

            @pl.when(on_line(z))
            def _():
                each(
                    0, CHUNKS, lambda c: arrived(line_recv.at[z, chunk(c)], line_r.at[z, c])
                )
                acc[...] += line_recv[z].astype(F32)

    mixed_ref[...] = acc[...].astype(BF16)

    def arrived_gin(s):
        p = mate(s)
        arrived(gin_all.at[p], gin_r.at[p])

    each(1, nd, arrived_gin)
    gin_ref[0] = jnp.sum(gin_all[...], axis=0)[:, 0:hidden].astype(BF16)

    def arrived_go(s):
        p = mate(s)

        @pl.when(p < parts)
        def _():
            arrived(go_buf.at[:, cols(p)], go_r.at[p])

    each(1, nd, arrived_go)
    gout_ref[0] = go_buf[...]

    def drain(s):
        gate_copy(s).wait_send()
        lg_copy(s).wait_send()
        rk_copy(peer(s)).wait_send()

        @pl.when(owner)
        def _():
            au_copy(s).wait_send()
            ge_copy(s).wait_send()

    each(1, n, drain)

    def drain_line(z):
        def piece(c):
            @pl.when((z <= at_line) & (at_line + 1 < line))
            def _():
                up_copy(z, c).wait_send()

            @pl.when((z >= at_line) & (at_line >= 1))
            def _():
                down_copy(z, c).wait_send()

            @pl.when(crosses(z))
            def _():
                each(1, side, lambda s: side_copy(z, s, c).wait_send())

            @pl.when((z == at_line) & outer)
            def _():
                each(1, side, lambda s: onward_copy(s, c).wait_send())

            @pl.when((z == at_line) | (z - at_line >= 2) | (at_line - z >= 2))
            def _():
                each(1, side, lambda s: pair_copy(z, other(s), c).wait_send())

            @pl.when((z - at_line >= 2) | (at_line - z >= 2))
            def _():
                line_copy(z, c).wait_send()

        each(0, CHUNKS, piece)

        @pl.when((z - at_line == 1) | (at_line - z == 1))
        def _():
            each(0, side, lambda x: near_copy(z, x).wait_send())

    each(0, line, drain_line)

    def drain_mates(s):
        gin_copy(s).wait_send()

        @pl.when(mate(s) < parts)
        def _():
            gm_copy(s).wait_send()

        @pl.when(owner)
        def _():
            am_copy(s).wait_send()
            go_copy(s).wait_send()

    each(1, nd, drain_mates)


def hand_over(a_ref, b_ref, c_ref, x_ref, y_ref, z_ref):
    x_ref[...] = a_ref[...]
    y_ref[...] = b_ref[...]
    z_ref[...] = c_ref[...]


def shards(
    n,
    nd,
    tokens,
    chosen_expert_index,
    router_gate_weight,
    output_gradient,
    gate_weight_matrix,
    up_weight,
    down_weight,
    adapter_down_maps,
    adapter_up_maps,
):
    rows, width = tokens.shape
    rank, hidden = adapter_down_maps.shape[1:]
    line = line_of(n)
    side = n // line
    parts = parts_of(nd, width)
    part = width // parts
    vmem = pl.BlockSpec(memory_space=pltpu.VMEM)
    anywhere = pl.BlockSpec(memory_space=pl.ANY)
    dma = pltpu.SemaphoreType.DMA
    results = pl.pallas_call(
        functools.partial(kernel, n, nd),
        out_shape=(
            jax.ShapeDtypeStruct((rows, width), BF16),
            jax.ShapeDtypeStruct((1, rank, hidden), BF16),
            jax.ShapeDtypeStruct((1, rank, width), BF16),
        ),
        in_specs=[anywhere, vmem, vmem, vmem, anywhere, anywhere, anywhere, vmem, anywhere],
        out_specs=(vmem, vmem, vmem),
        scratch_shapes=[
            pltpu.VMEM((n, rows, width), BF16),
            pltpu.VMEM((hidden, width), BF16),
            pltpu.VMEM((hidden, width), BF16),
            pltpu.VMEM((hidden + rank, width), BF16),
            pltpu.VMEM((n, rows, hidden + rank), BF16),
            pltpu.VMEM((n, rows, width), BF16),
            pltpu.VMEM((n, rows, width), BF16),
            pltpu.VMEM((2, side, rows, width), BF16),
            pltpu.VMEM((line, rows, width), BF16),
            pltpu.VMEM((line, rows, width), BF16),
            pltpu.VMEM((n, 1, rows), F32),
            pltpu.VMEM((n, rank, width), BF16),
            pltpu.VMEM((n, rank, rows), BF16),
            pltpu.VMEM((n, rank, rows), BF16),
            pltpu.VMEM((n, rank, rows), BF16),
            pltpu.VMEM((n, rank, rows), BF16),
            pltpu.VMEM((n, rank, rows), F32),
            pltpu.VMEM((n * rank, width), BF16),
            pltpu.VMEM((nd, n * rank, part), BF16),
            pltpu.VMEM((n, rank, part), BF16),
            pltpu.VMEM((n, rank, part), BF16),
            pltpu.VMEM((rank, width), BF16),
            pltpu.VMEM((nd, rank, hidden + rank), F32),
            pltpu.VMEM((rows, width), F32),
            dma((6,)),
        ]
        + [dma((line, CHUNKS))] * 2
        + [dma((n, CHUNKS)), dma((side, CHUNKS))]
        + [dma((n, CHUNKS))] * 3
        + [dma((2, side))] * 2
        + [dma((line, CHUNKS))] * 2
        + [dma((n,))] * 4
        + [dma((nd,))] * 2
        + [dma((n,))] * 4
        + [dma((nd,))] * 2
        + [dma((n,))] * 2
        + [dma((nd,))] * 4,
        compiler_params=pltpu.CompilerParams(
            collective_id=0, has_side_effects=True, vmem_limit_bytes=60 * 1024 * 1024
        ),
    )(
        tokens,
        chosen_expert_index.T,
        router_gate_weight.T,
        output_gradient,
        jnp.swapaxes(gate_weight_matrix, 1, 2),
        jnp.swapaxes(up_weight, 1, 2),
        down_weight,
        adapter_down_maps,
        adapter_up_maps,
    )
    return pl.pallas_call(
        hand_over,
        out_shape=tuple(jax.ShapeDtypeStruct(r.shape, r.dtype) for r in results),
        in_specs=[vmem] * 3,
        out_specs=(vmem,) * 3,
    )(*results)


def solution(mesh):
    return jax.shard_map(
        functools.partial(shards, mesh.shape["expert"], mesh.shape["dp"]),
        mesh=mesh,
        in_specs=(
            P(("dp", "expert"), None),
            P(("dp", "expert"), None),
            P(("dp", "expert"), None),
            P(("dp", "expert"), None),
            P("expert", None, None),
            P("expert", None, None),
            P("expert", None, None),
            P("expert", None, None),
            P("expert", None, None),
        ),
        out_specs=(P(("dp", "expert"), None), P("expert", None, None), P("expert", None, None)),
        check_vma=False,
    )
```

```python
import functools

import jax
import jax.numpy as jnp
from jax import lax
from jax.experimental import pallas as pl
from jax.experimental.pallas import tpu as pltpu
from jax.sharding import PartitionSpec as P

MESH = pl.DeviceIdType.MESH
F32 = jnp.float32
BF16 = jnp.bfloat16
CHUNKS = 2


def dot_nt(a, b):
    return lax.dot_general(a, b, (((1,), (1,)), ((), ())), preferred_element_type=F32)


def dot(a, b):
    return jnp.dot(a, b, preferred_element_type=F32)


def each(lo, hi, fn):
    def body(s, carry):
        fn(s)
        return carry

    lax.fori_loop(lo, hi, body, 0)


def line_of(n):
    assert n % 4 == 0
    return 4


OUTER = ((0, 0), (1, 0), (0, 1), (2, 0), (1, 1), (2, 1), (3, 0), (3, 1))
INNER = ((0, 0), (1, 0), (-1, 0), (0, 1), (1, 1), (-1, 1), (2, 1), (2, 0))
RELAYS = {1: ((1, 0), (1, 1)), 2: ((2, 0),), 3: ((2, 1),), 5: ((3, 0), (3, 1))}


def parts_of(nd, width):
    parts = 1
    while parts * 2 <= nd and width % (parts * 2 * 128) == 0:
        parts *= 2
    return parts


def kernel(
    n,
    nd,
    tok_h,
    idx_h,
    w_h,
    og_h,
    gw_h,
    uw_h,
    dw_h,
    ad_h,
    au_h,
    mixed_h,
    gin_h,
    gout_h,
    tok_all,
    idx_ref,
    w_ref,
    og_ref,
    ad_ref,
    gw,
    uw,
    dw,
    hid_all,
    term,
    pair_recv,
    near_recv,
    line_send,
    line_recv,
    gate_recv,
    au_all,
    lg_send,
    lg_recv,
    rk_send,
    rk_recv,
    gexp,
    gp_buf,
    gm_recv,
    ge_send,
    ge_recv,
    go_buf,
    gin_all,
    acc,
    mixed_ref,
    gin_ref,
    loc_sem,
    up_s,
    down_s,
    side_s,
    onward_s,
    tok_r,
    pair_s,
    pair_r,
    near_s,
    near_r,
    line_s,
    line_r,
    gate_s,
    gate_r,
    au_s,
    au_r,
    am_s,
    am_r,
    lg_s,
    lg_r,
    rk_s,
    rk_r,
    gm_s,
    gm_r,
    ge_s,
    ge_r,
    go_s,
    go_r,
    gin_s,
    gin_r,
):
    me = lax.axis_index("expert")
    rep = lax.axis_index("dp")
    line = line_of(n)
    side = n // line
    at_line = me // side
    at_side = lax.rem(me, side)
    rows = tok_all.shape[1]
    rank = ad_h.shape[1]
    width = tok_all.shape[2]
    hidden = ad_h.shape[2]
    parts = parts_of(nd, width)
    part = width // parts
    cr = rows // CHUNKS
    owner = rep < parts
    front = jnp.where(2 * at_line < line, 1, -1)
    outer = (at_line == 0) | (at_line == line - 1)

    def peer(s):
        return lax.rem(me + s, n)

    def mate(s):
        return lax.rem(rep + s, nd)

    def other(s):
        return lax.rem(at_side + s, side)

    def to_expert(src, dst, s_sem, r_sem, p):
        return pltpu.make_async_remote_copy(
            src_ref=src,
            dst_ref=dst,
            send_sem=s_sem,
            recv_sem=r_sem,
            device_id={"expert": p},
            device_id_type=MESH,
        )

    def to_mate(src, dst, s_sem, r_sem, p):
        return pltpu.make_async_remote_copy(
            src_ref=src,
            dst_ref=dst,
            send_sem=s_sem,
            recv_sem=r_sem,
            device_id={"dp": p},
            device_id_type=MESH,
        )

    def on_line(z):
        return (z >= 0) & (z < line)

    def chunk(c):
        return pl.ds(pl.multiple_of(c * cr, cr), cr)

    def cols(p):
        return pl.ds(pl.multiple_of(p * part, part), part)

    loads = [
        pltpu.make_async_copy(tok_h, tok_all.at[me], loc_sem.at[0]),
        pltpu.make_async_copy(gw_h.at[0], gw, loc_sem.at[1]),
        pltpu.make_async_copy(uw_h.at[0], uw, loc_sem.at[2]),
        pltpu.make_async_copy(dw_h.at[0], dw.at[pl.ds(0, hidden)], loc_sem.at[3]),
        pltpu.make_async_copy(au_h.at[0], dw.at[pl.ds(hidden, rank)], loc_sem.at[4]),
        pltpu.make_async_copy(ad_h.at[0], ad_ref, loc_sem.at[6]),
        pltpu.make_async_copy(og_h, og_ref, loc_sem.at[7]),
    ]
    tables = [
        pltpu.make_async_copy(idx_h, idx_ref, loc_sem.at[8]),
        pltpu.make_async_copy(w_h, w_ref, loc_sem.at[9]),
    ]
    for load in tables + loads:
        load.start()

    def load_map():
        return pltpu.make_async_copy(
            au_h.at[0, :, cols(rep)], au_all.at[me, :, cols(rep)], loc_sem.at[5]
        )

    @pl.when(owner)
    def _():
        load_map().start()

    barrier = pltpu.get_barrier_semaphore()
    each(
        1,
        n,
        lambda s: pl.semaphore_signal(
            barrier, inc=1, device_id={"expert": peer(s)}, device_id_type=MESH
        ),
    )
    each(
        1,
        nd,
        lambda s: pl.semaphore_signal(
            barrier, inc=1, device_id={"dp": mate(s)}, device_id_type=MESH
        ),
    )

    eye = lax.broadcasted_iota(jnp.int32, (rows, rows), 0) == lax.broadcasted_iota(
        jnp.int32, (rows, rows), 1
    )

    def spread_gates(e):
        row = jnp.sum(jnp.where(idx_ref[...] == e, w_ref[...], 0.0), axis=0, keepdims=True)
        gexp[e] = jnp.broadcast_to(row, (rank, rows))

    for load in tables:
        load.wait()
    each(0, n, spread_gates)
    gate_recv[me] = gexp[me, 0:1]

    def up_copy(z, c):
        k = z * side + at_side
        p = (at_line + 1) * side + at_side
        ref = tok_all.at[k, chunk(c)]
        return to_expert(ref, ref, up_s.at[z, c], tok_r.at[k, c], p)

    def down_copy(z, c):
        k = z * side + at_side
        p = (at_line - 1) * side + at_side
        ref = tok_all.at[k, chunk(c)]
        return to_expert(ref, ref, down_s.at[z, c], tok_r.at[k, c], p)

    def side_copy(z, s, c):
        k = z * side + at_side
        x = other(s)
        p = at_line * side + x
        ref = tok_all.at[k, chunk(c)]
        return to_expert(ref, ref, side_s.at[z * side + x, c], tok_r.at[k, c], p)

    def onward_copy(s, c):
        x = other(s)
        ref = tok_all.at[at_line * side + x, chunk(c)]
        p = (at_line + front) * side + at_side
        return to_expert(ref, ref, onward_s.at[x, c], tok_r.at[at_line * side + x, c], p)

    def gate_copy(s):
        p = peer(s)
        return to_expert(
            gexp.at[p, pl.ds(0, 1)], gate_recv.at[me], gate_s.at[p], gate_r.at[me], p
        )

    def au_copy(s):
        p = peer(s)
        ref = au_all.at[me, :, cols(rep)]
        return to_expert(ref, ref, au_s.at[p], au_r.at[me], p)

    def am_copy(s):
        p = mate(s)
        ref = au_all.at[:, :, cols(rep)]
        return to_mate(ref, ref, am_s.at[p], am_r.at[rep], p)

    def pair_copy(z, x, c):
        k = z * side + x
        p = at_line * side + x
        mine = z * side + at_side
        return to_expert(
            term.at[k, chunk(c)], pair_recv.at[mine, chunk(c)], pair_s.at[k, c],
            pair_r.at[mine, c], p,
        )

    def near_copy(z, x):
        b = jnp.where(z > at_line, 0, 1)
        p = z * side + at_side
        return to_expert(
            term.at[z * side + x], near_recv.at[b, x], near_s.at[b, x], near_r.at[b, x], p
        )

    def line_copy(z, c):
        p = z * side + at_side
        return to_expert(
            line_send.at[z, chunk(c)], line_recv.at[at_line, chunk(c)], line_s.at[z, c],
            line_r.at[at_line, c], p,
        )

    def lg_copy(s):
        p = peer(s)
        return to_expert(lg_send.at[p], lg_recv.at[me], lg_s.at[p], lg_r.at[me], p)

    def rk_copy(p):
        return to_expert(rk_send.at[p], rk_recv.at[me], rk_s.at[p], rk_r.at[me], p)

    def gm_copy(s):
        p = mate(s)
        return to_mate(gp_buf.at[:, cols(p)], gm_recv.at[rep], gm_s.at[p], gm_r.at[rep], p)

    def ge_copy(s):
        p = peer(s)
        return to_expert(ge_send.at[p], ge_recv.at[me], ge_s.at[p], ge_r.at[me], p)

    def go_copy(s):
        p = mate(s)
        ref = go_buf.at[:, cols(rep)]
        return to_mate(ref, ref, go_s.at[p], go_r.at[rep], p)

    def gin_copy(s):
        p = mate(s)
        return to_mate(gin_all.at[rep], gin_all.at[rep], gin_s.at[p], gin_r.at[rep], p)

    def arrived(ref, sem):
        to_expert(ref, ref, sem, sem, me).wait_recv()

    def arrived_tok(k, c):
        arrived(tok_all.at[k, chunk(c)], tok_r.at[k, c])

    def crosses(z):
        return outer | (z != at_line - front)

    def spread(z, c, go_up, go_down):
        @pl.when(crosses(z))
        def _():
            each(1, side, lambda s: side_copy(z, s, c).start())

        @pl.when(go_up & (at_line + 1 < line))
        def _():
            up_copy(z, c).start()

        @pl.when(go_down & (at_line >= 1))
        def _():
            down_copy(z, c).start()

    loads[0].wait()
    pl.semaphore_wait(barrier, n - 1 + nd - 1)

    each(1, n, lambda s: gate_copy(s).start())
    each(0, CHUNKS, lambda c: spread(at_line, c, True, True))
    for load in loads[1:]:
        load.wait()

    def send_maps():
        @pl.when(owner)
        def _():
            load_map().wait()
            each(1, n, lambda s: au_copy(s).start())

    def share_maps():
        @pl.when(owner)
        def _():
            def arrived_au(s):
                p = peer(s)
                arrived(au_all.at[p, :, cols(rep)], au_r.at[p])

            each(1, n, arrived_au)
            each(1, nd, lambda s: am_copy(s).start())

    def low_grads():
        def arrived_am(s):
            p = mate(s)

            @pl.when(p < parts)
            def _():
                arrived(au_all.at[:, :, cols(p)], am_r.at[p])

        each(1, nd, arrived_am)
        low_grad = dot_nt(au_all[...].reshape(n * rank, width), og_ref[...])
        low_grad = low_grad * gexp[...].reshape(n * rank, rows)
        lg_send[...] = low_grad.astype(BF16).reshape(n, rank, rows)
        lg_recv[me] = lg_send[me]
        each(1, n, lambda s: lg_copy(s).start())

    def relay(k, c):
        for sign in (-1, 1):
            z = at_line + sign * k

            @pl.when((k >= 1) & on_line(z))
            def _():
                arrived_tok(z * side + at_side, c)
                spread(z, c, sign < 0, sign > 0)

        @pl.when((k == 1) & outer)
        def _():
            def onward(s):
                arrived_tok(at_line * side + other(s), c)
                onward_copy(s, c).start()

            each(1, side, onward)

    def expert_block(src):
        x = tok_all[src]
        g = dot_nt(x, gw[...])
        u = dot_nt(x, uw[...])
        h = (g / (1.0 + jnp.exp(-g)) * u).astype(BF16)
        low = dot_nt(h, ad_ref[...])
        hid_all[src, :, 0:hidden] = h
        hid_all[src, :, hidden : hidden + rank] = low.astype(BF16)
        out = dot(hid_all[src], dw[...]).astype(BF16)
        return low.T.astype(BF16), out

    def work(dist, s):
        z = at_line + front * dist
        x = other(s)
        src = z * side + x

        def run():
            @pl.when((s > 0) & ((dist != 0) | ~outer))
            def _():
                each(0, CHUNKS, lambda c: arrived_tok(src, c))

            @pl.when(src != me)
            def _():
                arrived(gate_recv.at[src], gate_r.at[src])

            low_t, out = expert_block(src)
            row = gate_recv[src, 0:1]
            column = jnp.sum(jnp.where(eye, row, 0.0), axis=1, keepdims=True)
            term[src] = (out.astype(F32) * column).astype(BF16)

            @pl.when(src == me)
            def _():
                rk_recv[me] = low_t

            @pl.when(src != me)
            def _():
                rk_send[src] = low_t
                rk_copy(src).start()

            @pl.when((s > 0) & ((dist == 1) | (dist == -1)))
            def _():
                near_copy(z, x).start()

            @pl.when((s > 0) & (dist >= 2))
            def _():
                each(0, CHUNKS, lambda c: pair_copy(z, x, c).start())

        run()

    def near_own(z):
        @pl.when(on_line(z))
        def _():
            near_copy(z, at_side).start()

    def pick(i, values):
        total = 0
        for j, value in enumerate(values):
            total = total + value * (i == j).astype(jnp.int32)
        return total

    def step(i):
        for at, pieces in RELAYS.items():

            @pl.when(i == at)
            def _():
                for k, c in pieces:
                    relay(k, c)

        pl.when(i == 3)(lambda: near_own(at_line + front))
        pl.when(i == 5)(lambda: near_own(at_line - front))
        inner = 1 - outer.astype(jnp.int32)
        dist = pick(i, [d for d, _ in OUTER]) * (1 - inner) + pick(i, [d for d, _ in INNER]) * inner
        cross = pick(i, [c for _, c in OUTER]) * (1 - inner) + pick(i, [c for _, c in INNER]) * inner
        each(cross, 1 + cross * (side - 1), lambda s: work(dist, s))
        pl.when(i == 1)(send_maps)
        pl.when(i == 4)(share_maps)
        pl.when(i == 6)(low_grads)

    each(0, len(OUTER), step)

    def pairs(k, c):
        for sign in (-1, 1):
            z = at_line + sign * k

            @pl.when(on_line(z))
            def _():
                def piece():
                    def wait_pair(s):
                        src = z * side + other(s)
                        arrived(pair_recv.at[src, chunk(c)], pair_r.at[src, c])

                    each(1, side, wait_pair)

                    def add(s, total):
                        return total + pair_recv[z * side + other(s), chunk(c)].astype(F32)

                    total = lax.fori_loop(
                        1, side, add, term[z * side + at_side, chunk(c)].astype(F32)
                    )
                    line_send[z, chunk(c)] = total.astype(BF16)
                    line_copy(z, c).start()

                piece()

    def near_sum(x, total_ref):
        total_ref[...] = term[at_line * side + x].astype(F32)

        @pl.when(at_line >= 1)
        def _():
            arrived(near_recv.at[0, x], near_r.at[0, x])
            total_ref[...] += near_recv[0, x].astype(F32)

        @pl.when(at_line + 1 < line)
        def _():
            arrived(near_recv.at[1, x], near_r.at[1, x])
            total_ref[...] += near_recv[1, x].astype(F32)

    def merge(s):
        x = other(s)
        near_sum(x, acc)
        term[at_line * side + x] = acc[...].astype(BF16)

    def send_merged(c):
        each(1, side, lambda s: pair_copy(at_line, other(s), c).start())

    def in_grads():
        def arrived_lg(s):
            p = peer(s)
            arrived(lg_recv.at[p], lg_r.at[p])

        each(1, n, arrived_lg)

        def add_gin(src, total):
            return total + dot(lg_recv[src], hid_all[src])

        gin_all[rep] = lax.fori_loop(0, n, add_gin, jnp.zeros(gin_all.shape[1:], F32))
        each(1, nd, lambda s: gin_copy(s).start())

    def out_grads():
        def arrived_rk(s):
            p = peer(s)
            arrived(rk_recv.at[p], rk_r.at[p])

        each(1, n, arrived_rk)
        low_w = (rk_recv[...].astype(F32) * gexp[...]).astype(BF16).reshape(n * rank, rows)
        gp_buf[...] = dot(low_w, og_ref[...]).astype(BF16)

        def send(s):
            @pl.when(mate(s) < parts)
            def _():
                gm_copy(s).start()

        each(1, nd, send)

    def mate_sum():
        @pl.when(owner)
        def _():
            def add(s, total):
                p = mate(s)
                arrived(gm_recv.at[p], gm_r.at[p])
                return total + gm_recv[p].astype(F32)

            total = lax.fori_loop(1, nd, add, gp_buf[:, cols(rep)].astype(F32))
            ge_send[...] = total.astype(BF16).reshape(n, rank, part)
            each(1, n, lambda s: ge_copy(s).start())

    def expert_sum():
        @pl.when(owner)
        def _():
            def add(s, total):
                p = peer(s)
                arrived(ge_recv.at[p], ge_r.at[p])
                return total + ge_recv[p].astype(F32)

            total = lax.fori_loop(1, n, add, ge_send[me].astype(F32))
            go_buf[:, cols(rep)] = total.astype(BF16)
            each(1, nd, lambda s: go_copy(s).start())

    for c in range(CHUNKS):
        pairs(2, c)
    out_grads()
    for k in range(3, line):
        pairs(k, 0)
    each(1, side, merge)
    send_merged(0)
    pl.when(~outer)(lambda: each(1, CHUNKS, send_merged))
    mate_sum()
    for c in range(1, CHUNKS):
        for k in range(3, line):
            pairs(k, c)
        pl.when(outer)(lambda c=c: send_merged(c))
    in_grads()
    near_sum(at_side, acc)
    expert_sum()

    def add_merged(s):
        src = at_line * side + other(s)
        each(0, CHUNKS, lambda c: arrived(pair_recv.at[src, chunk(c)], pair_r.at[src, c]))
        acc[...] += pair_recv[src].astype(F32)

    each(1, side, add_merged)

    for k in range(2, line):
        for sign in (-1, 1):
            z = at_line + sign * k

            @pl.when(on_line(z))
            def _():
                each(
                    0, CHUNKS, lambda c: arrived(line_recv.at[z, chunk(c)], line_r.at[z, c])
                )
                acc[...] += line_recv[z].astype(F32)

    mixed_ref[...] = acc[...].astype(BF16)
    put_mixed = pltpu.make_async_copy(mixed_ref, mixed_h, loc_sem.at[0])
    put_gin = pltpu.make_async_copy(gin_ref, gin_h.at[0], loc_sem.at[1])
    put_gout = pltpu.make_async_copy(go_buf, gout_h.at[0], loc_sem.at[2])
    put_mixed.start()

    def arrived_gin(s):
        p = mate(s)
        arrived(gin_all.at[p], gin_r.at[p])

    each(1, nd, arrived_gin)
    gin_ref[...] = jnp.sum(gin_all[...], axis=0)[:, 0:hidden].astype(BF16)
    put_gin.start()

    def arrived_go(s):
        p = mate(s)

        @pl.when(p < parts)
        def _():
            arrived(go_buf.at[:, cols(p)], go_r.at[p])

    each(1, nd, arrived_go)
    put_gout.start()

    def drain(s):
        gate_copy(s).wait_send()
        lg_copy(s).wait_send()
        rk_copy(peer(s)).wait_send()

        @pl.when(owner)
        def _():
            au_copy(s).wait_send()
            ge_copy(s).wait_send()

    each(1, n, drain)

    def drain_line(z):
        def piece(c):
            @pl.when((z <= at_line) & (at_line + 1 < line))
            def _():
                up_copy(z, c).wait_send()

            @pl.when((z >= at_line) & (at_line >= 1))
            def _():
                down_copy(z, c).wait_send()

            @pl.when(crosses(z))
            def _():
                each(1, side, lambda s: side_copy(z, s, c).wait_send())

            @pl.when((z == at_line) & outer)
            def _():
                each(1, side, lambda s: onward_copy(s, c).wait_send())

            @pl.when((z == at_line) | (z - at_line >= 2) | (at_line - z >= 2))
            def _():
                each(1, side, lambda s: pair_copy(z, other(s), c).wait_send())

            @pl.when((z - at_line >= 2) | (at_line - z >= 2))
            def _():
                line_copy(z, c).wait_send()

        each(0, CHUNKS, piece)

        @pl.when((z - at_line == 1) | (at_line - z == 1))
        def _():
            each(0, side, lambda x: near_copy(z, x).wait_send())

    each(0, line, drain_line)

    def drain_mates(s):
        gin_copy(s).wait_send()

        @pl.when(mate(s) < parts)
        def _():
            gm_copy(s).wait_send()

        @pl.when(owner)
        def _():
            am_copy(s).wait_send()
            go_copy(s).wait_send()

    each(1, nd, drain_mates)
    put_mixed.wait()
    put_gin.wait()
    put_gout.wait()


def hand_over(a_ref, b_ref, c_ref, x_ref, y_ref, z_ref):
    x_ref[...] = a_ref[...]
    y_ref[...] = b_ref[...]
    z_ref[...] = c_ref[...]


def shards(
    n,
    nd,
    tokens,
    chosen_expert_index,
    router_gate_weight,
    output_gradient,
    gate_weight_matrix,
    up_weight,
    down_weight,
    adapter_down_maps,
    adapter_up_maps,
):
    rows, width = tokens.shape
    rank, hidden = adapter_down_maps.shape[1:]
    line = line_of(n)
    side = n // line
    parts = parts_of(nd, width)
    part = width // parts
    vmem = pl.BlockSpec(memory_space=pltpu.VMEM)
    hbm = pl.BlockSpec(memory_space=pltpu.HBM)
    dma = pltpu.SemaphoreType.DMA
    results = pl.pallas_call(
        functools.partial(kernel, n, nd),
        out_shape=(
            jax.ShapeDtypeStruct((rows, width), BF16),
            jax.ShapeDtypeStruct((1, rank, hidden), BF16),
            jax.ShapeDtypeStruct((1, rank, width), BF16),
        ),
        in_specs=[hbm] * 9,
        out_specs=(hbm,) * 3,
        scratch_shapes=[
            pltpu.VMEM((n, rows, width), BF16),
            pltpu.VMEM(chosen_expert_index.shape[::-1], jnp.int32),
            pltpu.VMEM(router_gate_weight.shape[::-1], F32),
            pltpu.VMEM((rows, width), BF16),
            pltpu.VMEM((rank, hidden), BF16),
            pltpu.VMEM((hidden, width), BF16),
            pltpu.VMEM((hidden, width), BF16),
            pltpu.VMEM((hidden + rank, width), BF16),
            pltpu.VMEM((n, rows, hidden + rank), BF16),
            pltpu.VMEM((n, rows, width), BF16),
            pltpu.VMEM((n, rows, width), BF16),
            pltpu.VMEM((2, side, rows, width), BF16),
            pltpu.VMEM((line, rows, width), BF16),
            pltpu.VMEM((line, rows, width), BF16),
            pltpu.VMEM((n, 1, rows), F32),
            pltpu.VMEM((n, rank, width), BF16),
            pltpu.VMEM((n, rank, rows), BF16),
            pltpu.VMEM((n, rank, rows), BF16),
            pltpu.VMEM((n, rank, rows), BF16),
            pltpu.VMEM((n, rank, rows), BF16),
            pltpu.VMEM((n, rank, rows), F32),
            pltpu.VMEM((n * rank, width), BF16),
            pltpu.VMEM((nd, n * rank, part), BF16),
            pltpu.VMEM((n, rank, part), BF16),
            pltpu.VMEM((n, rank, part), BF16),
            pltpu.VMEM((rank, width), BF16),
            pltpu.VMEM((nd, rank, hidden + rank), F32),
            pltpu.VMEM((rows, width), F32),
            pltpu.VMEM((rows, width), BF16),
            pltpu.VMEM((rank, hidden), BF16),
            dma((10,)),
        ]
        + [dma((line, CHUNKS))] * 2
        + [dma((n, CHUNKS)), dma((side, CHUNKS))]
        + [dma((n, CHUNKS))] * 3
        + [dma((2, side))] * 2
        + [dma((line, CHUNKS))] * 2
        + [dma((n,))] * 4
        + [dma((nd,))] * 2
        + [dma((n,))] * 4
        + [dma((nd,))] * 2
        + [dma((n,))] * 2
        + [dma((nd,))] * 4,
        compiler_params=pltpu.CompilerParams(
            collective_id=0, has_side_effects=True, vmem_limit_bytes=60 * 1024 * 1024
        ),
    )(
        tokens,
        chosen_expert_index.T,
        router_gate_weight.T,
        output_gradient,
        jnp.swapaxes(gate_weight_matrix, 1, 2),
        jnp.swapaxes(up_weight, 1, 2),
        down_weight,
        adapter_down_maps,
        adapter_up_maps,
    )
    return pl.pallas_call(
        hand_over,
        out_shape=tuple(jax.ShapeDtypeStruct(r.shape, r.dtype) for r in results),
        in_specs=[vmem] * 3,
        out_specs=(vmem,) * 3,
    )(*results)


def solution(mesh):
    return jax.shard_map(
        functools.partial(shards, mesh.shape["expert"], mesh.shape["dp"]),
        mesh=mesh,
        in_specs=(
            P(("dp", "expert"), None),
            P(("dp", "expert"), None),
            P(("dp", "expert"), None),
            P(("dp", "expert"), None),
            P("expert", None, None),
            P("expert", None, None),
            P("expert", None, None),
            P("expert", None, None),
            P("expert", None, None),
        ),
        out_specs=(P(("dp", "expert"), None), P("expert", None, None), P("expert", None, None)),
        check_vma=False,
    )
```

```python
import functools

import jax
import jax.numpy as jnp
from jax import lax
from jax.experimental import pallas as pl
from jax.experimental.pallas import tpu as pltpu
from jax.sharding import PartitionSpec as P

MESH = pl.DeviceIdType.MESH
F32 = jnp.float32
BF16 = jnp.bfloat16
CHUNKS = 2


def dot_nt(a, b):
    return lax.dot_general(a, b, (((1,), (1,)), ((), ())), preferred_element_type=F32)


def dot(a, b):
    return jnp.dot(a, b, preferred_element_type=F32)


def each(lo, hi, fn):
    def body(s, carry):
        fn(s)
        return carry

    lax.fori_loop(lo, hi, body, 0)


def line_of(n):
    assert n % 4 == 0
    return 4


OUTER = ((0, 0), (1, 0), (0, 1), (2, 0), (1, 1), (2, 1), (3, 0), (3, 1))
INNER = ((0, 0), (1, 0), (-1, 0), (0, 1), (1, 1), (2, 0), (2, 1), (-1, 1))
RELAYS = {1: ((1, 0), (1, 1)), 2: ((2, 0),), 3: ((2, 1),), 4: ((3, 0),), 5: ((3, 1),)}


def parts_of(nd, width):
    parts = 1
    while parts * 2 <= nd and width % (parts * 2 * 128) == 0:
        parts *= 2
    return parts


def kernel(
    n,
    nd,
    tok_h,
    idx_h,
    w_h,
    og_h,
    gw_h,
    uw_h,
    dw_h,
    ad_h,
    au_h,
    mixed_h,
    gin_h,
    gout_h,
    tok_all,
    idx_ref,
    w_ref,
    og_ref,
    ad_ref,
    gw,
    uw,
    dw,
    hid_all,
    term,
    pair_recv,
    near_recv,
    line_send,
    line_recv,
    gate_recv,
    au_all,
    lg_send,
    lg_recv,
    rk_send,
    rk_recv,
    gexp,
    gp_buf,
    gm_recv,
    ge_send,
    ge_recv,
    go_buf,
    gin_all,
    acc,
    mixed_ref,
    gin_ref,
    meet_sem,
    loc_sem,
    up_s,
    down_s,
    side_s,
    onward_s,
    tok_r,
    pair_s,
    pair_r,
    near_s,
    near_r,
    line_s,
    line_r,
    gate_s,
    gate_r,
    au_s,
    au_r,
    am_s,
    am_r,
    lg_s,
    lg_r,
    rk_s,
    rk_r,
    gm_s,
    gm_r,
    ge_s,
    ge_r,
    go_s,
    go_r,
    gin_s,
    gin_r,
):
    me = lax.axis_index("expert")
    rep = lax.axis_index("dp")
    line = line_of(n)
    side = n // line
    at_line = me // side
    at_side = lax.rem(me, side)
    rows = tok_all.shape[1]
    rank = ad_h.shape[1]
    width = tok_all.shape[2]
    hidden = ad_h.shape[2]
    parts = parts_of(nd, width)
    part = width // parts
    cr = rows // CHUNKS
    owner = rep < parts
    front = jnp.where(2 * at_line < line, 1, -1)
    outer = (at_line == 0) | (at_line == line - 1)

    def peer(s):
        return lax.rem(me + s, n)

    def mate(s):
        return lax.rem(rep + s, nd)

    def other(s):
        return lax.rem(at_side + s, side)

    def to_expert(src, dst, s_sem, r_sem, p):
        return pltpu.make_async_remote_copy(
            src_ref=src,
            dst_ref=dst,
            send_sem=s_sem,
            recv_sem=r_sem,
            device_id={"expert": p},
            device_id_type=MESH,
        )

    def to_mate(src, dst, s_sem, r_sem, p):
        return pltpu.make_async_remote_copy(
            src_ref=src,
            dst_ref=dst,
            send_sem=s_sem,
            recv_sem=r_sem,
            device_id={"dp": p},
            device_id_type=MESH,
        )

    def on_line(z):
        return (z >= 0) & (z < line)

    def chunk(c):
        return pl.ds(pl.multiple_of(c * cr, cr), cr)

    def cols(p):
        return pl.ds(pl.multiple_of(p * part, part), part)

    loads = [
        pltpu.make_async_copy(tok_h, tok_all.at[me], loc_sem.at[0]),
        pltpu.make_async_copy(gw_h.at[0], gw, loc_sem.at[1]),
        pltpu.make_async_copy(uw_h.at[0], uw, loc_sem.at[2]),
        pltpu.make_async_copy(dw_h.at[0], dw.at[pl.ds(0, hidden)], loc_sem.at[3]),
        pltpu.make_async_copy(au_h.at[0], dw.at[pl.ds(hidden, rank)], loc_sem.at[4]),
        pltpu.make_async_copy(ad_h.at[0], ad_ref, loc_sem.at[6]),
        pltpu.make_async_copy(og_h, og_ref, loc_sem.at[7]),
    ]
    tables = [
        pltpu.make_async_copy(idx_h, idx_ref, loc_sem.at[8]),
        pltpu.make_async_copy(w_h, w_ref, loc_sem.at[9]),
    ]
    for load in tables + loads:
        load.start()

    def load_map():
        return pltpu.make_async_copy(
            au_h.at[0, :, cols(rep)], au_all.at[me, :, cols(rep)], loc_sem.at[5]
        )

    @pl.when(owner)
    def _():
        load_map().start()

    barrier = pltpu.get_barrier_semaphore()

    def greet(sem, p):
        pl.semaphore_signal(sem, inc=1, device_id={"expert": p}, device_id_type=MESH)

    def greet_sides(sem):
        each(1, side, lambda s: greet(sem, at_line * side + other(s)))

    above, below = at_line + 1 < line, at_line >= 1
    greet_sides(barrier)
    pl.when(above)(lambda: greet(barrier, me + side))
    pl.when(below)(lambda: greet(barrier, me - side))
    each(
        1,
        nd,
        lambda s: pl.semaphore_signal(
            barrier, inc=1, device_id={"dp": mate(s)}, device_id_type=MESH
        ),
    )

    eye = lax.broadcasted_iota(jnp.int32, (rows, rows), 0) == lax.broadcasted_iota(
        jnp.int32, (rows, rows), 1
    )

    def spread_gates(e):
        row = jnp.sum(jnp.where(idx_ref[...] == e, w_ref[...], 0.0), axis=0, keepdims=True)
        gexp[e] = jnp.broadcast_to(row, (rank, rows))

    for load in tables:
        load.wait()
    each(0, n, spread_gates)
    gate_recv[me] = gexp[me, 0:1]

    def up_copy(z, c):
        k = z * side + at_side
        p = (at_line + 1) * side + at_side
        ref = tok_all.at[k, chunk(c)]
        return to_expert(ref, ref, up_s.at[z, c], tok_r.at[k, c], p)

    def down_copy(z, c):
        k = z * side + at_side
        p = (at_line - 1) * side + at_side
        ref = tok_all.at[k, chunk(c)]
        return to_expert(ref, ref, down_s.at[z, c], tok_r.at[k, c], p)

    def side_copy(z, s, c):
        k = z * side + at_side
        x = other(s)
        p = at_line * side + x
        ref = tok_all.at[k, chunk(c)]
        return to_expert(ref, ref, side_s.at[z * side + x, c], tok_r.at[k, c], p)

    def onward_copy(s, c):
        x = other(s)
        ref = tok_all.at[at_line * side + x, chunk(c)]
        p = (at_line + front) * side + at_side
        return to_expert(ref, ref, onward_s.at[x, c], tok_r.at[at_line * side + x, c], p)

    def gate_copy(s):
        p = peer(s)
        return to_expert(
            gexp.at[p, pl.ds(0, 1)], gate_recv.at[me], gate_s.at[p], gate_r.at[me], p
        )

    def au_copy(s):
        p = peer(s)
        ref = au_all.at[me, :, cols(rep)]
        return to_expert(ref, ref, au_s.at[p], au_r.at[me], p)

    def am_copy(s):
        p = mate(s)
        ref = au_all.at[:, :, cols(rep)]
        return to_mate(ref, ref, am_s.at[p], am_r.at[rep], p)

    def pair_copy(z, x, c):
        k = z * side + x
        p = at_line * side + x
        mine = z * side + at_side
        return to_expert(
            term.at[k, chunk(c)], pair_recv.at[mine, chunk(c)], pair_s.at[k, c],
            pair_r.at[mine, c], p,
        )

    def near_copy(z, x):
        b = jnp.where(z > at_line, 0, 1)
        p = z * side + at_side
        return to_expert(
            term.at[z * side + x], near_recv.at[b, x], near_s.at[b, x], near_r.at[b, x], p
        )

    def line_copy(z, c):
        p = z * side + at_side
        return to_expert(
            line_send.at[z, chunk(c)], line_recv.at[at_line, chunk(c)], line_s.at[z, c],
            line_r.at[at_line, c], p,
        )

    def lg_copy(s):
        p = peer(s)
        return to_expert(lg_send.at[p], lg_recv.at[me], lg_s.at[p], lg_r.at[me], p)

    def rk_copy(p):
        return to_expert(rk_send.at[p], rk_recv.at[me], rk_s.at[p], rk_r.at[me], p)

    def gm_copy(s):
        p = mate(s)
        return to_mate(gp_buf.at[:, cols(p)], gm_recv.at[rep], gm_s.at[p], gm_r.at[rep], p)

    def ge_copy(s):
        p = peer(s)
        return to_expert(ge_send.at[p], ge_recv.at[me], ge_s.at[p], ge_r.at[me], p)

    def go_copy(s):
        p = mate(s)
        ref = go_buf.at[:, cols(rep)]
        return to_mate(ref, ref, go_s.at[p], go_r.at[rep], p)

    def gin_copy(s):
        p = mate(s)
        return to_mate(gin_all.at[rep], gin_all.at[rep], gin_s.at[p], gin_r.at[rep], p)

    def arrived(ref, sem):
        to_expert(ref, ref, sem, sem, me).wait_recv()

    def arrived_tok(k, c):
        arrived(tok_all.at[k, chunk(c)], tok_r.at[k, c])

    def far(a, b):
        return (a - b >= 2) | (b - a >= 2)

    def crosses(z):
        return outer | (z != at_line - front)

    def spread(z, c, go_up, go_down):
        @pl.when(crosses(z))
        def _():
            each(1, side, lambda s: side_copy(z, s, c).start())

        @pl.when(go_up & (at_line + 1 < line))
        def _():
            up_copy(z, c).start()

        @pl.when(go_down & (at_line >= 1))
        def _():
            down_copy(z, c).start()

    loads[0].wait()
    neighbours = side - 1 + above.astype(jnp.int32) + below.astype(jnp.int32)
    pl.semaphore_wait(barrier, neighbours + nd - 1)

    def meet_all():
        pl.when(below)(lambda: pl.semaphore_wait(meet_sem.at[0], 1))
        pl.when(above)(lambda: greet(meet_sem.at[0], me + side))
        pl.when(above)(lambda: pl.semaphore_wait(meet_sem.at[1], 1))
        pl.when(below)(lambda: greet(meet_sem.at[1], me - side))
        greet_sides(meet_sem.at[2])
        pl.semaphore_wait(meet_sem.at[2], side - 1)
        each(1, n, lambda s: gate_copy(s).start())

    each(0, CHUNKS, lambda c: spread(at_line, c, True, True))
    for load in loads[1:]:
        load.wait()

    def send_maps():
        @pl.when(owner)
        def _():
            load_map().wait()
            each(1, n, lambda s: au_copy(s).start())

    def share_maps():
        @pl.when(owner)
        def _():
            def arrived_au(s):
                p = peer(s)
                arrived(au_all.at[p, :, cols(rep)], au_r.at[p])

            each(1, n, arrived_au)
            each(1, nd, lambda s: am_copy(s).start())

    def low_grads():
        def arrived_am(s):
            p = mate(s)

            @pl.when(p < parts)
            def _():
                arrived(au_all.at[:, :, cols(p)], am_r.at[p])

        each(1, nd, arrived_am)
        low_grad = dot_nt(au_all[...].reshape(n * rank, width), og_ref[...])
        low_grad = low_grad * gexp[...].reshape(n * rank, rows)
        lg_send[...] = low_grad.astype(BF16).reshape(n, rank, rows)
        lg_recv[me] = lg_send[me]
        each(1, n, lambda s: lg_copy(s).start())

    def relay(k, c):
        for sign in (-1, 1):
            z = at_line + sign * k

            @pl.when((k >= 1) & on_line(z))
            def _():
                arrived_tok(z * side + at_side, c)
                spread(z, c, sign < 0, sign > 0)

        @pl.when((k == 1) & outer)
        def _():
            def onward(s):
                arrived_tok(at_line * side + other(s), c)
                onward_copy(s, c).start()

            each(1, side, onward)

    def expert_block(src):
        x = tok_all[src]
        g = dot_nt(x, gw[...])
        u = dot_nt(x, uw[...])
        h = (g / (1.0 + jnp.exp(-g)) * u).astype(BF16)
        low = dot_nt(h, ad_ref[...])
        hid_all[src, :, 0:hidden] = h
        hid_all[src, :, hidden : hidden + rank] = low.astype(BF16)
        out = dot(hid_all[src], dw[...]).astype(BF16)
        return low.T.astype(BF16), out

    def work(dist, s):
        z = at_line + front * dist
        x = other(s)
        src = z * side + x

        def run():
            @pl.when((s > 0) & ((dist != 0) | ~outer))
            def _():
                each(0, CHUNKS, lambda c: arrived_tok(src, c))

            @pl.when(src != me)
            def _():
                arrived(gate_recv.at[src], gate_r.at[src])

            low_t, out = expert_block(src)
            row = gate_recv[src, 0:1]
            column = jnp.sum(jnp.where(eye, row, 0.0), axis=1, keepdims=True)
            term[src] = (out.astype(F32) * column).astype(BF16)

            @pl.when(src == me)
            def _():
                rk_recv[me] = low_t

            @pl.when(src != me)
            def _():
                rk_send[src] = low_t
                rk_copy(src).start()

            @pl.when((s > 0) & (dist == 1))
            def _():
                near_copy(z, x).start()

            last = jnp.where(outer & (dist == 2), 1, CHUNKS)

            @pl.when((s > 0) & (dist >= 2))
            def _():
                each(0, last, lambda c: pair_copy(z, x, c).start())

            @pl.when((s > 0) & (dist == 3))
            def _():
                each(1, CHUNKS, lambda c: pair_copy(z - front, x, c).start())

        run()

    def near_own(z):
        @pl.when(on_line(z))
        def _():
            near_copy(z, at_side).start()

    def near_sum(x, total_ref):
        total_ref[...] = term[at_line * side + x].astype(F32)

        @pl.when((at_line >= 1) & (2 * (at_line - 1) < line))
        def _():
            arrived(near_recv.at[0, x], near_r.at[0, x])
            total_ref[...] += near_recv[0, x].astype(F32)

        @pl.when((at_line + 1 < line) & (2 * (at_line + 1) >= line))
        def _():
            arrived(near_recv.at[1, x], near_r.at[1, x])
            total_ref[...] += near_recv[1, x].astype(F32)

    def merge(s):
        x = other(s)
        near_sum(x, acc)
        term[at_line * side + x] = acc[...].astype(BF16)

    def send_merged(c):
        each(1, side, lambda s: pair_copy(at_line, other(s), c).start())

    def pick(i, values):
        total = 0
        for j, value in enumerate(values):
            total = total + value * (i == j).astype(jnp.int32)
        return total

    def step(i):
        for at, pieces in RELAYS.items():

            @pl.when(i == at)
            def _():
                for k, c in pieces:
                    relay(k, c)

        pl.when(i == 3)(lambda: near_own(at_line + front))
        pl.when((i == 7) & outer)(lambda: send_merged(0))
        inner = 1 - outer.astype(jnp.int32)
        dist = pick(i, [d for d, _ in OUTER]) * (1 - inner) + pick(i, [d for d, _ in INNER]) * inner
        cross = pick(i, [c for _, c in OUTER]) * (1 - inner) + pick(i, [c for _, c in INNER]) * inner
        each(cross, 1 + cross * (side - 1), lambda s: work(dist, s))
        pl.when(i == 0)(meet_all)
        pl.when(i == 1)(send_maps)
        pl.when(i == 4)(share_maps)
        pl.when(i == 6)(low_grads)

    each(0, len(OUTER), step)

    def pairs(dist, c):
        z = at_line + front * dist

        @pl.when(on_line(z))
        def _():
            def wait_pair(s):
                src = z * side + other(s)
                arrived(pair_recv.at[src, chunk(c)], pair_r.at[src, c])

            each(1, side, wait_pair)

            def add(s, total):
                return total + pair_recv[z * side + other(s), chunk(c)].astype(F32)

            total = lax.fori_loop(1, side, add, term[z * side + at_side, chunk(c)].astype(F32))
            line_send[z, chunk(c)] = total.astype(BF16)
            line_copy(z, c).start()

    def late_pairs(c):
        pairs(jnp.where(outer, line - 1, -1), c)

    def in_grads():
        def arrived_lg(s):
            p = peer(s)
            arrived(lg_recv.at[p], lg_r.at[p])

        each(1, n, arrived_lg)

        def add_gin(src, total):
            return total + dot(lg_recv[src], hid_all[src])

        gin_all[rep] = lax.fori_loop(0, n, add_gin, jnp.zeros(gin_all.shape[1:], F32))
        each(1, nd, lambda s: gin_copy(s).start())

    def out_grads():
        def arrived_rk(s):
            p = peer(s)
            arrived(rk_recv.at[p], rk_r.at[p])

        each(1, n, arrived_rk)
        low_w = (rk_recv[...].astype(F32) * gexp[...]).astype(BF16).reshape(n * rank, rows)
        gp_buf[...] = dot(low_w, og_ref[...]).astype(BF16)

        def send(s):
            @pl.when(mate(s) < parts)
            def _():
                gm_copy(s).start()

        each(1, nd, send)

    def mate_sum():
        @pl.when(owner)
        def _():
            def add(s, total):
                p = mate(s)
                arrived(gm_recv.at[p], gm_r.at[p])
                return total + gm_recv[p].astype(F32)

            total = lax.fori_loop(1, nd, add, gp_buf[:, cols(rep)].astype(F32))
            ge_send[...] = total.astype(BF16).reshape(n, rank, part)
            each(1, n, lambda s: ge_copy(s).start())

    def expert_sum():
        @pl.when(owner)
        def _():
            def add(s, total):
                p = peer(s)
                arrived(ge_recv.at[p], ge_r.at[p])
                return total + ge_recv[p].astype(F32)

            total = lax.fori_loop(1, n, add, ge_send[me].astype(F32))
            go_buf[:, cols(rep)] = total.astype(BF16)
            each(1, nd, lambda s: go_copy(s).start())

    def send_back(s):
        each(0, CHUNKS, lambda c: pair_copy(at_line - front, other(s), c).start())

    pairs(2, 0)
    pl.when(~outer)(lambda: each(1, side, send_back))
    pl.when(~outer)(lambda: each(1, CHUNKS, lambda c: pairs(2, c)))
    out_grads()
    late_pairs(0)
    mate_sum()
    each(1, CHUNKS, late_pairs)
    pl.when(outer)(lambda: each(1, CHUNKS, lambda c: pairs(2, c)))
    pl.when(outer)(lambda: each(1, CHUNKS, send_merged))
    pl.when(~outer)(lambda: each(1, side, merge))
    pl.when(~outer)(lambda: each(0, CHUNKS, send_merged))
    in_grads()
    near_sum(at_side, acc)
    expert_sum()

    def add_merged(s):
        src = at_line * side + other(s)
        each(0, CHUNKS, lambda c: arrived(pair_recv.at[src, chunk(c)], pair_r.at[src, c]))
        acc[...] += pair_recv[src].astype(F32)

    each(1, side, add_merged)

    def add_line(z):
        @pl.when(far(at_line, z) | (outer & (z == at_line + front)))
        def _():
            each(0, CHUNKS, lambda c: arrived(line_recv.at[z, chunk(c)], line_r.at[z, c]))
            acc[...] += line_recv[z].astype(F32)

    each(0, line, add_line)
    mixed_ref[...] = acc[...].astype(BF16)
    put_mixed = pltpu.make_async_copy(mixed_ref, mixed_h, loc_sem.at[0])
    put_gin = pltpu.make_async_copy(gin_ref, gin_h.at[0], loc_sem.at[1])
    put_gout = pltpu.make_async_copy(go_buf, gout_h.at[0], loc_sem.at[2])
    put_mixed.start()

    def arrived_gin(s):
        p = mate(s)
        arrived(gin_all.at[p], gin_r.at[p])

    each(1, nd, arrived_gin)
    gin_ref[...] = jnp.sum(gin_all[...], axis=0)[:, 0:hidden].astype(BF16)
    put_gin.start()

    def arrived_go(s):
        p = mate(s)

        @pl.when(p < parts)
        def _():
            arrived(go_buf.at[:, cols(p)], go_r.at[p])

    each(1, nd, arrived_go)
    put_gout.start()

    def drain(s):
        gate_copy(s).wait_send()
        lg_copy(s).wait_send()
        rk_copy(peer(s)).wait_send()

        @pl.when(owner)
        def _():
            au_copy(s).wait_send()
            ge_copy(s).wait_send()

    each(1, n, drain)

    def drain_line(z):
        def piece(c):
            @pl.when((z <= at_line) & (at_line + 1 < line))
            def _():
                up_copy(z, c).wait_send()

            @pl.when((z >= at_line) & (at_line >= 1))
            def _():
                down_copy(z, c).wait_send()

            @pl.when(crosses(z))
            def _():
                each(1, side, lambda s: side_copy(z, s, c).wait_send())

            @pl.when((z == at_line) & outer)
            def _():
                each(1, side, lambda s: onward_copy(s, c).wait_send())

            lined = far(at_line, z) | (~outer & (z == at_line - front))

            @pl.when((z == at_line) | lined)
            def _():
                each(1, side, lambda s: pair_copy(z, other(s), c).wait_send())

            @pl.when(lined)
            def _():
                line_copy(z, c).wait_send()

        each(0, CHUNKS, piece)

        @pl.when(z == at_line + front)
        def _():
            each(0, side, lambda x: near_copy(z, x).wait_send())

    each(0, line, drain_line)

    def drain_mates(s):
        gin_copy(s).wait_send()

        @pl.when(mate(s) < parts)
        def _():
            gm_copy(s).wait_send()

        @pl.when(owner)
        def _():
            am_copy(s).wait_send()
            go_copy(s).wait_send()

    each(1, nd, drain_mates)
    put_mixed.wait()
    put_gin.wait()
    put_gout.wait()


def hand_over(a_ref, b_ref, c_ref, x_ref, y_ref, z_ref):
    x_ref[...] = a_ref[...]
    y_ref[...] = b_ref[...]
    z_ref[...] = c_ref[...]


def shards(
    n,
    nd,
    tokens,
    chosen_expert_index,
    router_gate_weight,
    output_gradient,
    gate_weight_matrix,
    up_weight,
    down_weight,
    adapter_down_maps,
    adapter_up_maps,
):
    rows, width = tokens.shape
    rank, hidden = adapter_down_maps.shape[1:]
    line = line_of(n)
    side = n // line
    parts = parts_of(nd, width)
    part = width // parts
    vmem = pl.BlockSpec(memory_space=pltpu.VMEM)
    hbm = pl.BlockSpec(memory_space=pltpu.HBM)
    dma = pltpu.SemaphoreType.DMA
    results = pl.pallas_call(
        functools.partial(kernel, n, nd),
        out_shape=(
            jax.ShapeDtypeStruct((rows, width), BF16),
            jax.ShapeDtypeStruct((1, rank, hidden), BF16),
            jax.ShapeDtypeStruct((1, rank, width), BF16),
        ),
        in_specs=[hbm] * 9,
        out_specs=(hbm,) * 3,
        scratch_shapes=[
            pltpu.VMEM((n, rows, width), BF16),
            pltpu.VMEM(chosen_expert_index.shape[::-1], jnp.int32),
            pltpu.VMEM(router_gate_weight.shape[::-1], F32),
            pltpu.VMEM((rows, width), BF16),
            pltpu.VMEM((rank, hidden), BF16),
            pltpu.VMEM((hidden, width), BF16),
            pltpu.VMEM((hidden, width), BF16),
            pltpu.VMEM((hidden + rank, width), BF16),
            pltpu.VMEM((n, rows, hidden + rank), BF16),
            pltpu.VMEM((n, rows, width), BF16),
            pltpu.VMEM((n, rows, width), BF16),
            pltpu.VMEM((2, side, rows, width), BF16),
            pltpu.VMEM((line, rows, width), BF16),
            pltpu.VMEM((line, rows, width), BF16),
            pltpu.VMEM((n, 1, rows), F32),
            pltpu.VMEM((n, rank, width), BF16),
            pltpu.VMEM((n, rank, rows), BF16),
            pltpu.VMEM((n, rank, rows), BF16),
            pltpu.VMEM((n, rank, rows), BF16),
            pltpu.VMEM((n, rank, rows), BF16),
            pltpu.VMEM((n, rank, rows), F32),
            pltpu.VMEM((n * rank, width), BF16),
            pltpu.VMEM((nd, n * rank, part), BF16),
            pltpu.VMEM((n, rank, part), BF16),
            pltpu.VMEM((n, rank, part), BF16),
            pltpu.VMEM((rank, width), BF16),
            pltpu.VMEM((nd, rank, hidden + rank), F32),
            pltpu.VMEM((rows, width), F32),
            pltpu.VMEM((rows, width), BF16),
            pltpu.VMEM((rank, hidden), BF16),
            pltpu.SemaphoreType.REGULAR((3,)),
            dma((10,)),
        ]
        + [dma((line, CHUNKS))] * 2
        + [dma((n, CHUNKS)), dma((side, CHUNKS))]
        + [dma((n, CHUNKS))] * 3
        + [dma((2, side))] * 2
        + [dma((line, CHUNKS))] * 2
        + [dma((n,))] * 4
        + [dma((nd,))] * 2
        + [dma((n,))] * 4
        + [dma((nd,))] * 2
        + [dma((n,))] * 2
        + [dma((nd,))] * 4,
        compiler_params=pltpu.CompilerParams(
            collective_id=0, has_side_effects=True, vmem_limit_bytes=60 * 1024 * 1024
        ),
    )(
        tokens,
        chosen_expert_index.T,
        router_gate_weight.T,
        output_gradient,
        jnp.swapaxes(gate_weight_matrix, 1, 2),
        jnp.swapaxes(up_weight, 1, 2),
        down_weight,
        adapter_down_maps,
        adapter_up_maps,
    )
    return pl.pallas_call(
        hand_over,
        out_shape=tuple(jax.ShapeDtypeStruct(r.shape, r.dtype) for r in results),
        in_specs=[vmem] * 3,
        out_specs=(vmem,) * 3,
    )(*results)


def solution(mesh):
    return jax.shard_map(
        functools.partial(shards, mesh.shape["expert"], mesh.shape["dp"]),
        mesh=mesh,
        in_specs=(
            P(("dp", "expert"), None),
            P(("dp", "expert"), None),
            P(("dp", "expert"), None),
            P(("dp", "expert"), None),
            P("expert", None, None),
            P("expert", None, None),
            P("expert", None, None),
            P("expert", None, None),
            P("expert", None, None),
        ),
        out_specs=(P(("dp", "expert"), None), P("expert", None, None), P("expert", None, None)),
        check_vma=False,
    )
```

```python
import functools

import jax
import jax.numpy as jnp
from jax import lax
from jax.experimental import pallas as pl
from jax.experimental.pallas import tpu as pltpu
from jax.sharding import PartitionSpec as P

MESH = pl.DeviceIdType.MESH
F32 = jnp.float32
BF16 = jnp.bfloat16
CHUNKS = 2


def dot_nt(a, b):
    return lax.dot_general(a, b, (((1,), (1,)), ((), ())), preferred_element_type=F32)


def dot(a, b):
    return jnp.dot(a, b, preferred_element_type=F32)


def each(lo, hi, fn):
    def body(s, carry):
        fn(s)
        return carry

    lax.fori_loop(lo, hi, body, 0)


def line_of(n):
    assert n % 4 == 0
    return 4


OUTER = ((0, 0), (1, 0), (0, 1), (2, 0), (1, 1), (2, 1), (3, 0), (3, 1))
INNER = ((0, 0), (1, 0), (-1, 0), (0, 1), (1, 1), (2, 0), (2, 1), (-1, 1))
RELAYS = {1: ((1, 0), (1, 1)), 2: ((2, 0),), 3: ((2, 1),), 4: ((3, 0),), 5: ((3, 1),)}


def parts_of(nd, width):
    parts = 1
    while parts * 2 <= nd and width % (parts * 2 * 128) == 0:
        parts *= 2
    return parts


def kernel(
    n,
    nd,
    tok_h,
    idx_h,
    w_h,
    og_h,
    gw_h,
    uw_h,
    dw_h,
    ad_h,
    au_h,
    mixed_h,
    gin_h,
    gout_h,
    tok_all,
    idx_ref,
    w_ref,
    og_ref,
    ad_ref,
    gw,
    uw,
    dw,
    hid_all,
    term,
    pair_recv,
    near_recv,
    line_send,
    line_recv,
    gate_recv,
    au_all,
    lg_send,
    lg_recv,
    rk_send,
    rk_recv,
    gexp,
    gp_buf,
    gm_recv,
    ge_send,
    ge_recv,
    go_buf,
    gin_all,
    acc,
    mixed_ref,
    gin_ref,
    meet_sem,
    loc_sem,
    up_s,
    down_s,
    side_s,
    onward_s,
    tok_r,
    pair_s,
    pair_r,
    near_s,
    near_r,
    line_s,
    line_r,
    gate_s,
    gate_r,
    au_s,
    au_r,
    am_s,
    am_r,
    lg_s,
    lg_r,
    rk_s,
    rk_r,
    gm_s,
    gm_r,
    ge_s,
    ge_r,
    go_s,
    go_r,
    gin_s,
    gin_r,
):
    me = lax.axis_index("expert")
    rep = lax.axis_index("dp")
    line = line_of(n)
    side = n // line
    at_line = me // side
    at_side = lax.rem(me, side)
    rows = tok_all.shape[1]
    rank = ad_h.shape[1]
    width = tok_all.shape[2]
    hidden = ad_h.shape[2]
    parts = parts_of(nd, width)
    part = width // parts
    cr = rows // CHUNKS
    owner = rep < parts
    front = jnp.where(2 * at_line < line, 1, -1)
    outer = (at_line == 0) | (at_line == line - 1)

    def peer(s):
        return lax.rem(me + s, n)

    def mate(s):
        return lax.rem(rep + s, nd)

    def other(s):
        return lax.rem(at_side + s, side)

    def to_expert(src, dst, s_sem, r_sem, p):
        return pltpu.make_async_remote_copy(
            src_ref=src,
            dst_ref=dst,
            send_sem=s_sem,
            recv_sem=r_sem,
            device_id={"expert": p},
            device_id_type=MESH,
        )

    def to_mate(src, dst, s_sem, r_sem, p):
        return pltpu.make_async_remote_copy(
            src_ref=src,
            dst_ref=dst,
            send_sem=s_sem,
            recv_sem=r_sem,
            device_id={"dp": p},
            device_id_type=MESH,
        )

    def on_line(z):
        return (z >= 0) & (z < line)

    def chunk(c):
        return pl.ds(pl.multiple_of(c * cr, cr), cr)

    def cols(p):
        return pl.ds(pl.multiple_of(p * part, part), part)

    loads = [
        pltpu.make_async_copy(tok_h, tok_all.at[me], loc_sem.at[0]),
        pltpu.make_async_copy(gw_h.at[0], gw, loc_sem.at[1]),
        pltpu.make_async_copy(uw_h.at[0], uw, loc_sem.at[2]),
        pltpu.make_async_copy(dw_h.at[0], dw.at[pl.ds(0, hidden)], loc_sem.at[3]),
        pltpu.make_async_copy(au_h.at[0], dw.at[pl.ds(hidden, rank)], loc_sem.at[4]),
        pltpu.make_async_copy(ad_h.at[0], ad_ref, loc_sem.at[6]),
        pltpu.make_async_copy(og_h, og_ref, loc_sem.at[7]),
    ]
    tables = [
        pltpu.make_async_copy(idx_h, idx_ref, loc_sem.at[8]),
        pltpu.make_async_copy(w_h, w_ref, loc_sem.at[9]),
    ]
    for load in tables + loads:
        load.start()

    def load_map():
        return pltpu.make_async_copy(
            au_h.at[0, :, cols(rep)], au_all.at[me, :, cols(rep)], loc_sem.at[5]
        )

    @pl.when(owner)
    def _():
        load_map().start()

    barrier = pltpu.get_barrier_semaphore()

    def greet(sem, p):
        pl.semaphore_signal(sem, inc=1, device_id={"expert": p}, device_id_type=MESH)

    def greet_sides(sem):
        each(1, side, lambda s: greet(sem, at_line * side + other(s)))

    above, below = at_line + 1 < line, at_line >= 1
    greet_sides(barrier)
    pl.when(above)(lambda: greet(barrier, me + side))
    pl.when(below)(lambda: greet(barrier, me - side))
    each(
        1,
        nd,
        lambda s: pl.semaphore_signal(
            barrier, inc=1, device_id={"dp": mate(s)}, device_id_type=MESH
        ),
    )

    eye = lax.broadcasted_iota(jnp.int32, (rows, rows), 0) == lax.broadcasted_iota(
        jnp.int32, (rows, rows), 1
    )

    def spread_gates(e):
        row = jnp.sum(jnp.where(idx_ref[...] == e, w_ref[...], 0.0), axis=0, keepdims=True)
        gexp[e] = jnp.broadcast_to(row, (rank, rows))


    def up_copy(z, c):
        k = z * side + at_side
        p = (at_line + 1) * side + at_side
        ref = tok_all.at[k, chunk(c)]
        return to_expert(ref, ref, up_s.at[z, c], tok_r.at[k, c], p)

    def down_copy(z, c):
        k = z * side + at_side
        p = (at_line - 1) * side + at_side
        ref = tok_all.at[k, chunk(c)]
        return to_expert(ref, ref, down_s.at[z, c], tok_r.at[k, c], p)

    def side_copy(z, s, c):
        k = z * side + at_side
        x = other(s)
        p = at_line * side + x
        ref = tok_all.at[k, chunk(c)]
        return to_expert(ref, ref, side_s.at[z * side + x, c], tok_r.at[k, c], p)

    def onward_copy(s, c):
        x = other(s)
        ref = tok_all.at[at_line * side + x, chunk(c)]
        p = (at_line + front) * side + at_side
        return to_expert(ref, ref, onward_s.at[x, c], tok_r.at[at_line * side + x, c], p)

    def gate_copy(s):
        p = peer(s)
        return to_expert(
            gexp.at[p, pl.ds(0, 1)], gate_recv.at[me], gate_s.at[p], gate_r.at[me], p
        )

    def au_copy(s):
        p = peer(s)
        ref = au_all.at[me, :, cols(rep)]
        return to_expert(ref, ref, au_s.at[p], au_r.at[me], p)

    def am_copy(s):
        p = mate(s)
        ref = au_all.at[:, :, cols(rep)]
        return to_mate(ref, ref, am_s.at[p], am_r.at[rep], p)

    def pair_copy(z, x, c):
        k = z * side + x
        p = at_line * side + x
        mine = z * side + at_side
        return to_expert(
            term.at[k, chunk(c)], pair_recv.at[mine, chunk(c)], pair_s.at[k, c],
            pair_r.at[mine, c], p,
        )

    def near_copy(z, x):
        b = jnp.where(z > at_line, 0, 1)
        p = z * side + at_side
        return to_expert(
            term.at[z * side + x], near_recv.at[b, x], near_s.at[b, x], near_r.at[b, x], p
        )

    def line_copy(z, c):
        p = z * side + at_side
        return to_expert(
            line_send.at[z, chunk(c)], line_recv.at[at_line, chunk(c)], line_s.at[z, c],
            line_r.at[at_line, c], p,
        )

    def lg_copy(s):
        p = peer(s)
        return to_expert(lg_send.at[p], lg_recv.at[me], lg_s.at[p], lg_r.at[me], p)

    def rk_copy(p):
        return to_expert(rk_send.at[p], rk_recv.at[me], rk_s.at[p], rk_r.at[me], p)

    def gm_copy(s):
        p = mate(s)
        return to_mate(gp_buf.at[:, cols(p)], gm_recv.at[rep], gm_s.at[p], gm_r.at[rep], p)

    def ge_copy(s):
        p = peer(s)
        return to_expert(ge_send.at[p], ge_recv.at[me], ge_s.at[p], ge_r.at[me], p)

    def go_copy(s):
        p = mate(s)
        ref = go_buf.at[:, cols(rep)]
        return to_mate(ref, ref, go_s.at[p], go_r.at[rep], p)

    def gin_copy(s):
        p = mate(s)
        return to_mate(gin_all.at[rep], gin_all.at[rep], gin_s.at[p], gin_r.at[rep], p)

    def arrived(ref, sem):
        to_expert(ref, ref, sem, sem, me).wait_recv()

    def arrived_tok(k, c):
        arrived(tok_all.at[k, chunk(c)], tok_r.at[k, c])

    def far(a, b):
        return (a - b >= 2) | (b - a >= 2)

    def crosses(z):
        return outer | (z != at_line - front)

    def spread(z, c, go_up, go_down):
        @pl.when(crosses(z))
        def _():
            each(1, side, lambda s: side_copy(z, s, c).start())

        @pl.when(go_up & (at_line + 1 < line))
        def _():
            up_copy(z, c).start()

        @pl.when(go_down & (at_line >= 1))
        def _():
            down_copy(z, c).start()

    loads[0].wait()
    neighbours = side - 1 + above.astype(jnp.int32) + below.astype(jnp.int32)
    pl.semaphore_wait(barrier, neighbours + nd - 1)

    def meet_all():
        pl.when(below)(lambda: pl.semaphore_wait(meet_sem.at[0], 1))
        pl.when(above)(lambda: greet(meet_sem.at[0], me + side))
        pl.when(above)(lambda: pl.semaphore_wait(meet_sem.at[1], 1))
        pl.when(below)(lambda: greet(meet_sem.at[1], me - side))
        greet_sides(meet_sem.at[2])
        pl.semaphore_wait(meet_sem.at[2], side - 1)
        each(1, n, lambda s: gate_copy(s).start())

    each(0, CHUNKS, lambda c: spread(at_line, c, True, True))
    for load in tables:
        load.wait()
    each(0, n, spread_gates)
    gate_recv[me] = gexp[me, 0:1]
    for load in loads[1:]:
        load.wait()

    def send_maps():
        @pl.when(owner)
        def _():
            load_map().wait()
            each(1, n, lambda s: au_copy(s).start())

    def share_maps():
        @pl.when(owner)
        def _():
            def arrived_au(s):
                p = peer(s)
                arrived(au_all.at[p, :, cols(rep)], au_r.at[p])

            each(1, n, arrived_au)
            each(1, nd, lambda s: am_copy(s).start())

    def low_grads():
        def arrived_am(s):
            p = mate(s)

            @pl.when(p < parts)
            def _():
                arrived(au_all.at[:, :, cols(p)], am_r.at[p])

        each(1, nd, arrived_am)
        low_grad = dot_nt(au_all[...].reshape(n * rank, width), og_ref[...])
        low_grad = low_grad * gexp[...].reshape(n * rank, rows)
        lg_send[...] = low_grad.astype(BF16).reshape(n, rank, rows)
        lg_recv[me] = lg_send[me]
        each(1, n, lambda s: lg_copy(s).start())

    def relay(k, c):
        for sign in (-1, 1):
            z = at_line + sign * k

            @pl.when((k >= 1) & on_line(z))
            def _():
                arrived_tok(z * side + at_side, c)
                spread(z, c, sign < 0, sign > 0)

        @pl.when((k == 1) & outer)
        def _():
            def onward(s):
                arrived_tok(at_line * side + other(s), c)
                onward_copy(s, c).start()

            each(1, side, onward)

    def expert_block(src):
        x = tok_all[src]
        g = dot_nt(x, gw[...])
        u = dot_nt(x, uw[...])
        h = (g / (1.0 + jnp.exp(-g)) * u).astype(BF16)
        low = dot_nt(h, ad_ref[...])
        hid_all[src, :, 0:hidden] = h
        hid_all[src, :, hidden : hidden + rank] = low.astype(BF16)
        out = dot(hid_all[src], dw[...]).astype(BF16)
        return low.T.astype(BF16), out

    def work(dist, s):
        z = at_line + front * dist
        x = other(s)
        src = z * side + x

        def run():
            @pl.when((s > 0) & ((dist != 0) | ~outer))
            def _():
                each(0, CHUNKS, lambda c: arrived_tok(src, c))

            @pl.when(src != me)
            def _():
                arrived(gate_recv.at[src], gate_r.at[src])

            low_t, out = expert_block(src)
            row = gate_recv[src, 0:1]
            column = jnp.sum(jnp.where(eye, row, 0.0), axis=1, keepdims=True)
            term[src] = (out.astype(F32) * column).astype(BF16)

            @pl.when(src == me)
            def _():
                rk_recv[me] = low_t

            @pl.when(src != me)
            def _():
                rk_send[src] = low_t
                rk_copy(src).start()

            @pl.when((s > 0) & (dist == 1))
            def _():
                near_copy(z, x).start()

            last = jnp.where(outer & (dist == 2), 1, CHUNKS)

            @pl.when((s > 0) & (dist >= 2))
            def _():
                each(0, last, lambda c: pair_copy(z, x, c).start())

            @pl.when((s > 0) & (dist == 3))
            def _():
                each(1, CHUNKS, lambda c: pair_copy(z - front, x, c).start())

        run()

    def near_own(z):
        @pl.when(on_line(z))
        def _():
            near_copy(z, at_side).start()

    def near_sum(x, total_ref):
        total_ref[...] = term[at_line * side + x].astype(F32)

        @pl.when((at_line >= 1) & (2 * (at_line - 1) < line))
        def _():
            arrived(near_recv.at[0, x], near_r.at[0, x])
            total_ref[...] += near_recv[0, x].astype(F32)

        @pl.when((at_line + 1 < line) & (2 * (at_line + 1) >= line))
        def _():
            arrived(near_recv.at[1, x], near_r.at[1, x])
            total_ref[...] += near_recv[1, x].astype(F32)

    def merge(s):
        x = other(s)
        near_sum(x, acc)
        term[at_line * side + x] = acc[...].astype(BF16)

    def send_merged(c):
        each(1, side, lambda s: pair_copy(at_line, other(s), c).start())

    def pick(i, values):
        total = 0
        for j, value in enumerate(values):
            total = total + value * (i == j).astype(jnp.int32)
        return total

    def step(i):
        for at, pieces in RELAYS.items():

            @pl.when(i == at)
            def _():
                for k, c in pieces:
                    relay(k, c)

        pl.when(i == 3)(lambda: near_own(at_line + front))
        pl.when((i == 7) & outer)(lambda: send_merged(0))
        inner = 1 - outer.astype(jnp.int32)
        dist = pick(i, [d for d, _ in OUTER]) * (1 - inner) + pick(i, [d for d, _ in INNER]) * inner
        cross = pick(i, [c for _, c in OUTER]) * (1 - inner) + pick(i, [c for _, c in INNER]) * inner
        each(cross, 1 + cross * (side - 1), lambda s: work(dist, s))
        pl.when(i == 0)(meet_all)
        pl.when(i == 1)(send_maps)
        pl.when(i == 4)(share_maps)
        pl.when(i == 6)(low_grads)

    each(0, len(OUTER), step)

    def pairs(dist, c):
        z = at_line + front * dist

        @pl.when(on_line(z))
        def _():
            def wait_pair(s):
                src = z * side + other(s)
                arrived(pair_recv.at[src, chunk(c)], pair_r.at[src, c])

            each(1, side, wait_pair)

            def add(s, total):
                return total + pair_recv[z * side + other(s), chunk(c)].astype(F32)

            total = lax.fori_loop(1, side, add, term[z * side + at_side, chunk(c)].astype(F32))
            line_send[z, chunk(c)] = total.astype(BF16)
            line_copy(z, c).start()

    def late_pairs(c):
        pairs(jnp.where(outer, line - 1, -1), c)

    def in_grads():
        def arrived_lg(s):
            p = peer(s)
            arrived(lg_recv.at[p], lg_r.at[p])

        each(1, n, arrived_lg)

        def add_gin(src, total):
            return total + dot(lg_recv[src], hid_all[src])

        gin_all[rep] = lax.fori_loop(0, n, add_gin, jnp.zeros(gin_all.shape[1:], F32))
        each(1, nd, lambda s: gin_copy(s).start())

    def out_grads():
        def arrived_rk(s):
            p = peer(s)
            arrived(rk_recv.at[p], rk_r.at[p])

        each(1, n, arrived_rk)
        low_w = (rk_recv[...].astype(F32) * gexp[...]).astype(BF16).reshape(n * rank, rows)
        gp_buf[...] = dot(low_w, og_ref[...]).astype(BF16)

        def send(s):
            @pl.when(mate(s) < parts)
            def _():
                gm_copy(s).start()

        each(1, nd, send)

    def mate_sum():
        @pl.when(owner)
        def _():
            def add(s, total):
                p = mate(s)
                arrived(gm_recv.at[p], gm_r.at[p])
                return total + gm_recv[p].astype(F32)

            total = lax.fori_loop(1, nd, add, gp_buf[:, cols(rep)].astype(F32))
            ge_send[...] = total.astype(BF16).reshape(n, rank, part)
            each(1, n, lambda s: ge_copy(s).start())

    def expert_sum():
        @pl.when(owner)
        def _():
            def add(s, total):
                p = peer(s)
                arrived(ge_recv.at[p], ge_r.at[p])
                return total + ge_recv[p].astype(F32)

            total = lax.fori_loop(1, n, add, ge_send[me].astype(F32))
            go_buf[:, cols(rep)] = total.astype(BF16)
            each(1, nd, lambda s: go_copy(s).start())

    def send_back(s):
        each(0, CHUNKS, lambda c: pair_copy(at_line - front, other(s), c).start())

    pl.when(~outer)(lambda: each(1, side, send_back))
    pairs(2, 0)
    pl.when(~outer)(lambda: each(1, CHUNKS, lambda c: pairs(2, c)))
    out_grads()
    late_pairs(0)
    mate_sum()
    each(1, CHUNKS, late_pairs)
    pl.when(outer)(lambda: each(1, CHUNKS, lambda c: pairs(2, c)))
    pl.when(outer)(lambda: each(1, CHUNKS, send_merged))
    pl.when(~outer)(lambda: each(1, side, merge))
    pl.when(~outer)(lambda: each(0, CHUNKS, send_merged))
    in_grads()
    near_sum(at_side, acc)
    expert_sum()

    def add_merged(s):
        src = at_line * side + other(s)
        each(0, CHUNKS, lambda c: arrived(pair_recv.at[src, chunk(c)], pair_r.at[src, c]))
        acc[...] += pair_recv[src].astype(F32)

    each(1, side, add_merged)

    def add_line(z):
        @pl.when(far(at_line, z) | (outer & (z == at_line + front)))
        def _():
            each(0, CHUNKS, lambda c: arrived(line_recv.at[z, chunk(c)], line_r.at[z, c]))
            acc[...] += line_recv[z].astype(F32)

    each(0, line, add_line)
    mixed_ref[...] = acc[...].astype(BF16)
    put_mixed = pltpu.make_async_copy(mixed_ref, mixed_h, loc_sem.at[0])
    put_gin = pltpu.make_async_copy(gin_ref, gin_h.at[0], loc_sem.at[1])
    put_gout = pltpu.make_async_copy(go_buf, gout_h.at[0], loc_sem.at[2])
    put_mixed.start()

    def arrived_gin(s):
        p = mate(s)
        arrived(gin_all.at[p], gin_r.at[p])

    each(1, nd, arrived_gin)
    gin_ref[...] = jnp.sum(gin_all[...], axis=0)[:, 0:hidden].astype(BF16)
    put_gin.start()

    def arrived_go(s):
        p = mate(s)

        @pl.when(p < parts)
        def _():
            arrived(go_buf.at[:, cols(p)], go_r.at[p])

    each(1, nd, arrived_go)
    put_gout.start()

    def drain(s):
        gate_copy(s).wait_send()
        lg_copy(s).wait_send()
        rk_copy(peer(s)).wait_send()

        @pl.when(owner)
        def _():
            au_copy(s).wait_send()
            ge_copy(s).wait_send()

    each(1, n, drain)

    def drain_line(z):
        def piece(c):
            @pl.when((z <= at_line) & (at_line + 1 < line))
            def _():
                up_copy(z, c).wait_send()

            @pl.when((z >= at_line) & (at_line >= 1))
            def _():
                down_copy(z, c).wait_send()

            @pl.when(crosses(z))
            def _():
                each(1, side, lambda s: side_copy(z, s, c).wait_send())

            @pl.when((z == at_line) & outer)
            def _():
                each(1, side, lambda s: onward_copy(s, c).wait_send())

            lined = far(at_line, z) | (~outer & (z == at_line - front))

            @pl.when((z == at_line) | lined)
            def _():
                each(1, side, lambda s: pair_copy(z, other(s), c).wait_send())

            @pl.when(lined)
            def _():
                line_copy(z, c).wait_send()

        each(0, CHUNKS, piece)

        @pl.when(z == at_line + front)
        def _():
            each(0, side, lambda x: near_copy(z, x).wait_send())

    each(0, line, drain_line)

    def drain_mates(s):
        gin_copy(s).wait_send()

        @pl.when(mate(s) < parts)
        def _():
            gm_copy(s).wait_send()

        @pl.when(owner)
        def _():
            am_copy(s).wait_send()
            go_copy(s).wait_send()

    each(1, nd, drain_mates)
    put_mixed.wait()
    put_gin.wait()
    put_gout.wait()


def hand_over(a_ref, b_ref, c_ref, x_ref, y_ref, z_ref):
    x_ref[...] = a_ref[...]
    y_ref[...] = b_ref[...]
    z_ref[...] = c_ref[...]


def shards(
    n,
    nd,
    tokens,
    chosen_expert_index,
    router_gate_weight,
    output_gradient,
    gate_weight_matrix,
    up_weight,
    down_weight,
    adapter_down_maps,
    adapter_up_maps,
):
    rows, width = tokens.shape
    rank, hidden = adapter_down_maps.shape[1:]
    line = line_of(n)
    side = n // line
    parts = parts_of(nd, width)
    part = width // parts
    vmem = pl.BlockSpec(memory_space=pltpu.VMEM)
    hbm = pl.BlockSpec(memory_space=pltpu.HBM)
    dma = pltpu.SemaphoreType.DMA
    results = pl.pallas_call(
        functools.partial(kernel, n, nd),
        out_shape=(
            jax.ShapeDtypeStruct((rows, width), BF16),
            jax.ShapeDtypeStruct((1, rank, hidden), BF16),
            jax.ShapeDtypeStruct((1, rank, width), BF16),
        ),
        in_specs=[hbm] * 9,
        out_specs=(hbm,) * 3,
        scratch_shapes=[
            pltpu.VMEM((n, rows, width), BF16),
            pltpu.VMEM(chosen_expert_index.shape[::-1], jnp.int32),
            pltpu.VMEM(router_gate_weight.shape[::-1], F32),
            pltpu.VMEM((rows, width), BF16),
            pltpu.VMEM((rank, hidden), BF16),
            pltpu.VMEM((hidden, width), BF16),
            pltpu.VMEM((hidden, width), BF16),
            pltpu.VMEM((hidden + rank, width), BF16),
            pltpu.VMEM((n, rows, hidden + rank), BF16),
            pltpu.VMEM((n, rows, width), BF16),
            pltpu.VMEM((n, rows, width), BF16),
            pltpu.VMEM((2, side, rows, width), BF16),
            pltpu.VMEM((line, rows, width), BF16),
            pltpu.VMEM((line, rows, width), BF16),
            pltpu.VMEM((n, 1, rows), F32),
            pltpu.VMEM((n, rank, width), BF16),
            pltpu.VMEM((n, rank, rows), BF16),
            pltpu.VMEM((n, rank, rows), BF16),
            pltpu.VMEM((n, rank, rows), BF16),
            pltpu.VMEM((n, rank, rows), BF16),
            pltpu.VMEM((n, rank, rows), F32),
            pltpu.VMEM((n * rank, width), BF16),
            pltpu.VMEM((nd, n * rank, part), BF16),
            pltpu.VMEM((n, rank, part), BF16),
            pltpu.VMEM((n, rank, part), BF16),
            pltpu.VMEM((rank, width), BF16),
            pltpu.VMEM((nd, rank, hidden + rank), F32),
            pltpu.VMEM((rows, width), F32),
            pltpu.VMEM((rows, width), BF16),
            pltpu.VMEM((rank, hidden), BF16),
            pltpu.SemaphoreType.REGULAR((3,)),
            dma((10,)),
        ]
        + [dma((line, CHUNKS))] * 2
        + [dma((n, CHUNKS)), dma((side, CHUNKS))]
        + [dma((n, CHUNKS))] * 3
        + [dma((2, side))] * 2
        + [dma((line, CHUNKS))] * 2
        + [dma((n,))] * 4
        + [dma((nd,))] * 2
        + [dma((n,))] * 4
        + [dma((nd,))] * 2
        + [dma((n,))] * 2
        + [dma((nd,))] * 4,
        compiler_params=pltpu.CompilerParams(
            collective_id=0, has_side_effects=True, vmem_limit_bytes=60 * 1024 * 1024
        ),
    )(
        tokens,
        chosen_expert_index.T,
        router_gate_weight.T,
        output_gradient,
        jnp.swapaxes(gate_weight_matrix, 1, 2),
        jnp.swapaxes(up_weight, 1, 2),
        down_weight,
        adapter_down_maps,
        adapter_up_maps,
    )
    return pl.pallas_call(
        hand_over,
        out_shape=tuple(jax.ShapeDtypeStruct(r.shape, r.dtype) for r in results),
        in_specs=[vmem] * 3,
        out_specs=(vmem,) * 3,
    )(*results)


def solution(mesh):
    return jax.shard_map(
        functools.partial(shards, mesh.shape["expert"], mesh.shape["dp"]),
        mesh=mesh,
        in_specs=(
            P(("dp", "expert"), None),
            P(("dp", "expert"), None),
            P(("dp", "expert"), None),
            P(("dp", "expert"), None),
            P("expert", None, None),
            P("expert", None, None),
            P("expert", None, None),
            P("expert", None, None),
            P("expert", None, None),
        ),
        out_specs=(P(("dp", "expert"), None), P("expert", None, None), P("expert", None, None)),
        check_vma=False,
    )
```

```python
import functools

import jax
import jax.numpy as jnp
from jax import lax
from jax.experimental import pallas as pl
from jax.experimental.pallas import tpu as pltpu
from jax.sharding import PartitionSpec as P

MESH = pl.DeviceIdType.MESH
F32 = jnp.float32
BF16 = jnp.bfloat16
CHUNKS = 2


def dot_nt(a, b):
    return lax.dot_general(a, b, (((1,), (1,)), ((), ())), preferred_element_type=F32)


def dot(a, b):
    return jnp.dot(a, b, preferred_element_type=F32)


def each(lo, hi, fn):
    def body(s, carry):
        fn(s)
        return carry

    lax.fori_loop(lo, hi, body, 0)


def line_of(n):
    assert n % 4 == 0
    return 4


OUTER = ((0, 0), (1, 0), (0, 1), (2, 0), (1, 1), (2, 1), (3, 0), (3, 1))
INNER = ((0, 0), (1, 0), (-1, 0), (0, 1), (1, 1), (2, 0), (2, 1), (-1, 1))
RELAYS = {1: ((1, 0), (1, 1)), 2: ((2, 0),), 3: ((2, 1),), 4: ((3, 0),), 5: ((3, 1),)}


def parts_of(nd, width):
    parts = 1
    while parts * 2 <= nd and width % (parts * 2 * 128) == 0:
        parts *= 2
    return parts


def kernel(
    n,
    nd,
    tok_h,
    idx_h,
    w_h,
    og_h,
    gw_h,
    uw_h,
    dw_h,
    ad_h,
    au_h,
    mixed_h,
    gin_h,
    gout_h,
    tok_all,
    idx_ref,
    w_ref,
    og_ref,
    ad_ref,
    gw,
    uw,
    dw,
    hid_all,
    term,
    pair_recv,
    near_recv,
    line_send,
    line_recv,
    gate_recv,
    au_all,
    lg_send,
    lg_recv,
    rk_send,
    rk_recv,
    gexp,
    gp_buf,
    gm_recv,
    ge_send,
    ge_recv,
    go_buf,
    gin_all,
    acc,
    mixed_ref,
    gin_ref,
    meet_sem,
    loc_sem,
    up_s,
    down_s,
    side_s,
    onward_s,
    tok_r,
    pair_s,
    pair_r,
    near_s,
    near_r,
    line_s,
    line_r,
    gate_s,
    gate_r,
    au_s,
    au_r,
    am_s,
    am_r,
    lg_s,
    lg_r,
    rk_s,
    rk_r,
    gm_s,
    gm_r,
    ge_s,
    ge_r,
    go_s,
    go_r,
    gin_s,
    gin_r,
):
    me = lax.axis_index("expert")
    rep = lax.axis_index("dp")
    line = line_of(n)
    side = n // line
    at_line = me // side
    at_side = lax.rem(me, side)
    rows = tok_all.shape[1]
    rank = ad_h.shape[1]
    width = tok_all.shape[2]
    hidden = ad_h.shape[2]
    parts = parts_of(nd, width)
    part = width // parts
    cr = rows // CHUNKS
    owner = rep < parts
    front = jnp.where(2 * at_line < line, 1, -1)
    outer = (at_line == 0) | (at_line == line - 1)

    def peer(s):
        return lax.rem(me + s, n)

    def mate(s):
        return lax.rem(rep + s, nd)

    def other(s):
        return lax.rem(at_side + s, side)

    def to_expert(src, dst, s_sem, r_sem, p):
        return pltpu.make_async_remote_copy(
            src_ref=src,
            dst_ref=dst,
            send_sem=s_sem,
            recv_sem=r_sem,
            device_id={"expert": p},
            device_id_type=MESH,
        )

    def to_mate(src, dst, s_sem, r_sem, p):
        return pltpu.make_async_remote_copy(
            src_ref=src,
            dst_ref=dst,
            send_sem=s_sem,
            recv_sem=r_sem,
            device_id={"dp": p},
            device_id_type=MESH,
        )

    def on_line(z):
        return (z >= 0) & (z < line)

    def chunk(c):
        return pl.ds(pl.multiple_of(c * cr, cr), cr)

    def cols(p):
        return pl.ds(pl.multiple_of(p * part, part), part)

    loads = [
        pltpu.make_async_copy(tok_h, tok_all.at[me], loc_sem.at[0]),
        pltpu.make_async_copy(gw_h.at[0], gw, loc_sem.at[1]),
        pltpu.make_async_copy(uw_h.at[0], uw, loc_sem.at[2]),
        pltpu.make_async_copy(dw_h.at[0], dw.at[pl.ds(0, hidden)], loc_sem.at[3]),
        pltpu.make_async_copy(au_h.at[0], dw.at[pl.ds(hidden, rank)], loc_sem.at[4]),
        pltpu.make_async_copy(ad_h.at[0], ad_ref, loc_sem.at[6]),
        pltpu.make_async_copy(og_h, og_ref, loc_sem.at[7]),
    ]
    tables = [
        pltpu.make_async_copy(idx_h, idx_ref, loc_sem.at[8]),
        pltpu.make_async_copy(w_h, w_ref, loc_sem.at[9]),
    ]
    for load in tables + loads:
        load.start()

    def load_map():
        return pltpu.make_async_copy(
            au_h.at[0, :, cols(rep)], au_all.at[me, :, cols(rep)], loc_sem.at[5]
        )

    @pl.when(owner)
    def _():
        load_map().start()

    barrier = pltpu.get_barrier_semaphore()

    def greet(sem, p):
        pl.semaphore_signal(sem, inc=1, device_id={"expert": p}, device_id_type=MESH)

    def greet_sides(sem):
        each(1, side, lambda s: greet(sem, at_line * side + other(s)))

    above, below = at_line + 1 < line, at_line >= 1
    greet_sides(barrier)
    pl.when(above)(lambda: greet(barrier, me + side))
    pl.when(below)(lambda: greet(barrier, me - side))
    each(
        1,
        nd,
        lambda s: pl.semaphore_signal(
            barrier, inc=1, device_id={"dp": mate(s)}, device_id_type=MESH
        ),
    )

    eye = lax.broadcasted_iota(jnp.int32, (rows, rows), 0) == lax.broadcasted_iota(
        jnp.int32, (rows, rows), 1
    )

    def spread_gates(e):
        row = jnp.sum(jnp.where(idx_ref[...] == e, w_ref[...], 0.0), axis=0, keepdims=True)
        gexp[e] = jnp.broadcast_to(row, (rank, rows))


    def up_copy(z, c):
        k = z * side + at_side
        p = (at_line + 1) * side + at_side
        ref = tok_all.at[k, chunk(c)]
        return to_expert(ref, ref, up_s.at[z, c], tok_r.at[k, c], p)

    def down_copy(z, c):
        k = z * side + at_side
        p = (at_line - 1) * side + at_side
        ref = tok_all.at[k, chunk(c)]
        return to_expert(ref, ref, down_s.at[z, c], tok_r.at[k, c], p)

    def side_copy(z, s, c):
        k = z * side + at_side
        x = other(s)
        p = at_line * side + x
        ref = tok_all.at[k, chunk(c)]
        return to_expert(ref, ref, side_s.at[z * side + x, c], tok_r.at[k, c], p)

    def onward_copy(s, c):
        x = other(s)
        ref = tok_all.at[at_line * side + x, chunk(c)]
        p = (at_line + front) * side + at_side
        return to_expert(ref, ref, onward_s.at[x, c], tok_r.at[at_line * side + x, c], p)

    def gate_copy(s):
        p = peer(s)
        return to_expert(
            gexp.at[p, pl.ds(0, 1)], gate_recv.at[me], gate_s.at[p], gate_r.at[me], p
        )

    def au_copy(s):
        p = peer(s)
        ref = au_all.at[me, :, cols(rep)]
        return to_expert(ref, ref, au_s.at[p], au_r.at[me], p)

    def am_copy(s):
        p = mate(s)
        ref = au_all.at[:, :, cols(rep)]
        return to_mate(ref, ref, am_s.at[p], am_r.at[rep], p)

    def pair_copy(z, x, c):
        k = z * side + x
        p = at_line * side + x
        mine = z * side + at_side
        return to_expert(
            term.at[k, chunk(c)], pair_recv.at[mine, chunk(c)], pair_s.at[k, c],
            pair_r.at[mine, c], p,
        )

    def near_copy(z, x):
        b = jnp.where(z > at_line, 0, 1)
        p = z * side + at_side
        return to_expert(
            term.at[z * side + x], near_recv.at[b, x], near_s.at[b, x], near_r.at[b, x], p
        )

    def line_copy(z, c):
        p = z * side + at_side
        return to_expert(
            line_send.at[z, chunk(c)], line_recv.at[at_line, chunk(c)], line_s.at[z, c],
            line_r.at[at_line, c], p,
        )

    def lg_copy(s):
        p = peer(s)
        return to_expert(lg_send.at[p], lg_recv.at[me], lg_s.at[p], lg_r.at[me], p)

    def rk_copy(p):
        return to_expert(rk_send.at[p], rk_recv.at[me], rk_s.at[p], rk_r.at[me], p)

    def gm_copy(s):
        p = mate(s)
        return to_mate(gp_buf.at[:, cols(p)], gm_recv.at[rep], gm_s.at[p], gm_r.at[rep], p)

    def ge_copy(s):
        p = peer(s)
        return to_expert(ge_send.at[p], ge_recv.at[me], ge_s.at[p], ge_r.at[me], p)

    def go_copy(s):
        p = mate(s)
        ref = go_buf.at[:, cols(rep)]
        return to_mate(ref, ref, go_s.at[p], go_r.at[rep], p)

    def gin_copy(s):
        p = mate(s)
        return to_mate(gin_all.at[rep], gin_all.at[rep], gin_s.at[p], gin_r.at[rep], p)

    def arrived(ref, sem):
        to_expert(ref, ref, sem, sem, me).wait_recv()

    def arrived_tok(k, c):
        arrived(tok_all.at[k, chunk(c)], tok_r.at[k, c])

    def far(a, b):
        return (a - b >= 2) | (b - a >= 2)

    def crosses(z):
        return outer | (z != at_line - front)

    def spread(z, c, go_up, go_down):
        @pl.when(crosses(z))
        def _():
            each(1, side, lambda s: side_copy(z, s, c).start())

        @pl.when(go_up & (at_line + 1 < line))
        def _():
            up_copy(z, c).start()

        @pl.when(go_down & (at_line >= 1))
        def _():
            down_copy(z, c).start()

    loads[0].wait()
    neighbours = side - 1 + above.astype(jnp.int32) + below.astype(jnp.int32)
    pl.semaphore_wait(barrier, neighbours + nd - 1)

    def meet_all():
        pl.when(below)(lambda: pl.semaphore_wait(meet_sem.at[0], 1))
        pl.when(above)(lambda: greet(meet_sem.at[0], me + side))
        pl.when(above)(lambda: pl.semaphore_wait(meet_sem.at[1], 1))
        pl.when(below)(lambda: greet(meet_sem.at[1], me - side))
        greet_sides(meet_sem.at[2])
        pl.semaphore_wait(meet_sem.at[2], side - 1)
        each(1, n, lambda s: gate_copy(s).start())

    each(0, CHUNKS, lambda c: spread(at_line, c, True, True))
    for load in tables:
        load.wait()
    each(0, n, spread_gates)
    gate_recv[me] = gexp[me, 0:1]
    for load in loads[1:]:
        load.wait()

    def send_maps():
        @pl.when(owner)
        def _():
            load_map().wait()
            each(1, n, lambda s: au_copy(s).start())

    def share_maps():
        @pl.when(owner)
        def _():
            def arrived_au(s):
                p = peer(s)
                arrived(au_all.at[p, :, cols(rep)], au_r.at[p])

            each(1, n, arrived_au)
            each(1, nd, lambda s: am_copy(s).start())

    def low_grads():
        def arrived_am(s):
            p = mate(s)

            @pl.when(p < parts)
            def _():
                arrived(au_all.at[:, :, cols(p)], am_r.at[p])

        each(1, nd, arrived_am)
        low_grad = dot_nt(au_all[...].reshape(n * rank, width), og_ref[...])
        low_grad = low_grad * gexp[...].reshape(n * rank, rows)
        lg_send[...] = low_grad.astype(BF16).reshape(n, rank, rows)
        lg_recv[me] = lg_send[me]
        each(1, n, lambda s: lg_copy(s).start())

    def relay(k, c):
        for sign in (-1, 1):
            z = at_line + sign * k

            @pl.when((k >= 1) & on_line(z))
            def _():
                arrived_tok(z * side + at_side, c)
                spread(z, c, sign < 0, sign > 0)

        @pl.when((k == 1) & outer)
        def _():
            def onward(s):
                arrived_tok(at_line * side + other(s), c)
                onward_copy(s, c).start()

            each(1, side, onward)

    def expert_block(src):
        x = tok_all[src]
        g = dot_nt(x, gw[...])
        u = dot_nt(x, uw[...])
        h = (g / (1.0 + jnp.exp(-g)) * u).astype(BF16)
        low = dot_nt(h, ad_ref[...])
        hid_all[src, :, 0:hidden] = h
        hid_all[src, :, hidden : hidden + rank] = low.astype(BF16)
        out = dot(hid_all[src], dw[...]).astype(BF16)
        return low.T.astype(BF16), out

    def work(dist, s):
        z = at_line + front * dist
        x = other(s)
        src = z * side + x

        def run():
            @pl.when((s > 0) & ((dist != 0) | ~outer))
            def _():
                each(0, CHUNKS, lambda c: arrived_tok(src, c))

            @pl.when(src != me)
            def _():
                arrived(gate_recv.at[src], gate_r.at[src])

            low_t, out = expert_block(src)
            row = gate_recv[src, 0:1]
            column = jnp.sum(jnp.where(eye, row, 0.0), axis=1, keepdims=True)
            term[src] = (out.astype(F32) * column).astype(BF16)

            @pl.when(src == me)
            def _():
                rk_recv[me] = low_t

            @pl.when(src != me)
            def _():
                rk_send[src] = low_t
                rk_copy(src).start()

            @pl.when((s > 0) & (dist == 1))
            def _():
                near_copy(z, x).start()

            last = jnp.where(outer & (dist == 2), 1, CHUNKS)

            @pl.when((s > 0) & (dist >= 2))
            def _():
                each(0, last, lambda c: pair_copy(z, x, c).start())

            @pl.when((s > 0) & (dist == 3))
            def _():
                each(1, CHUNKS, lambda c: pair_copy(z - front, x, c).start())

        run()

    def near_own(z):
        @pl.when(on_line(z))
        def _():
            near_copy(z, at_side).start()

    def near_sum(x, total_ref):
        total_ref[...] = term[at_line * side + x].astype(F32)

        @pl.when((at_line >= 1) & (2 * (at_line - 1) < line))
        def _():
            arrived(near_recv.at[0, x], near_r.at[0, x])
            total_ref[...] += near_recv[0, x].astype(F32)

        @pl.when((at_line + 1 < line) & (2 * (at_line + 1) >= line))
        def _():
            arrived(near_recv.at[1, x], near_r.at[1, x])
            total_ref[...] += near_recv[1, x].astype(F32)

    def merge(s):
        x = other(s)
        near_sum(x, acc)
        term[at_line * side + x] = acc[...].astype(BF16)

    def send_merged(c):
        each(1, side, lambda s: pair_copy(at_line, other(s), c).start())

    def pick(i, values):
        total = 0
        for j, value in enumerate(values):
            total = total + value * (i == j).astype(jnp.int32)
        return total

    def step(i):
        for at, pieces in RELAYS.items():

            @pl.when(i == at)
            def _():
                for k, c in pieces:
                    relay(k, c)

        pl.when(i == 3)(lambda: near_own(at_line + front))
        pl.when((i == 7) & outer)(lambda: send_merged(0))
        inner = 1 - outer.astype(jnp.int32)
        dist = pick(i, [d for d, _ in OUTER]) * (1 - inner) + pick(i, [d for d, _ in INNER]) * inner
        cross = pick(i, [c for _, c in OUTER]) * (1 - inner) + pick(i, [c for _, c in INNER]) * inner
        each(cross, 1 + cross * (side - 1), lambda s: work(dist, s))
        pl.when(i == 0)(meet_all)
        pl.when(i == 1)(send_maps)
        pl.when(i == 4)(share_maps)
        pl.when(i == 6)(low_grads)

    each(0, len(OUTER), step)

    def pairs(dist, c):
        z = at_line + front * dist

        @pl.when(on_line(z))
        def _():
            def wait_pair(s):
                src = z * side + other(s)
                arrived(pair_recv.at[src, chunk(c)], pair_r.at[src, c])

            each(1, side, wait_pair)

            def add(s, total):
                return total + pair_recv[z * side + other(s), chunk(c)].astype(F32)

            total = lax.fori_loop(1, side, add, term[z * side + at_side, chunk(c)].astype(F32))
            line_send[z, chunk(c)] = total.astype(BF16)
            line_copy(z, c).start()

    def late_pairs(c):
        pairs(jnp.where(outer, line - 1, -1), c)

    def in_grads():
        def arrived_lg(s):
            p = peer(s)
            arrived(lg_recv.at[p], lg_r.at[p])

        each(1, n, arrived_lg)

        def add_gin(src, total):
            return total + dot(lg_recv[src], hid_all[src])

        gin_all[rep] = lax.fori_loop(0, n, add_gin, jnp.zeros(gin_all.shape[1:], F32))
        each(1, nd, lambda s: gin_copy(s).start())

    def out_grads():
        def arrived_rk(s):
            p = peer(s)
            arrived(rk_recv.at[p], rk_r.at[p])

        each(1, n, arrived_rk)
        low_w = (rk_recv[...].astype(F32) * gexp[...]).astype(BF16).reshape(n * rank, rows)
        gp_buf[...] = dot(low_w, og_ref[...]).astype(BF16)

        def send(s):
            @pl.when(mate(s) < parts)
            def _():
                gm_copy(s).start()

        each(1, nd, send)

    def mate_sum():
        @pl.when(owner)
        def _():
            def add(s, total):
                p = mate(s)
                arrived(gm_recv.at[p], gm_r.at[p])
                return total + gm_recv[p].astype(F32)

            total = lax.fori_loop(1, nd, add, gp_buf[:, cols(rep)].astype(F32))
            ge_send[...] = total.astype(BF16).reshape(n, rank, part)
            each(1, n, lambda s: ge_copy(s).start())

    def expert_sum():
        @pl.when(owner)
        def _():
            def add(s, total):
                p = peer(s)
                arrived(ge_recv.at[p], ge_r.at[p])
                return total + ge_recv[p].astype(F32)

            total = lax.fori_loop(1, n, add, ge_send[me].astype(F32))
            go_buf[:, cols(rep)] = total.astype(BF16)
            each(1, nd, lambda s: go_copy(s).start())

    def send_back(s):
        each(0, CHUNKS, lambda c: pair_copy(at_line - front, other(s), c).start())

    pl.when(~outer)(lambda: each(1, side, send_back))
    pairs(2, 0)
    pl.when(~outer)(lambda: each(1, CHUNKS, lambda c: pairs(2, c)))
    out_grads()
    pl.when(~outer)(lambda: each(1, side, merge))
    pl.when(~outer)(lambda: send_merged(0))
    late_pairs(0)
    mate_sum()
    each(1, CHUNKS, late_pairs)
    pl.when(outer)(lambda: each(1, CHUNKS, lambda c: pairs(2, c)))
    each(1, CHUNKS, send_merged)
    in_grads()
    near_sum(at_side, acc)
    expert_sum()

    def add_merged(s):
        src = at_line * side + other(s)
        each(0, CHUNKS, lambda c: arrived(pair_recv.at[src, chunk(c)], pair_r.at[src, c]))
        acc[...] += pair_recv[src].astype(F32)

    each(1, side, add_merged)

    def add_line(z):
        @pl.when(far(at_line, z) | (outer & (z == at_line + front)))
        def _():
            each(0, CHUNKS, lambda c: arrived(line_recv.at[z, chunk(c)], line_r.at[z, c]))
            acc[...] += line_recv[z].astype(F32)

    each(0, line, add_line)
    mixed_ref[...] = acc[...].astype(BF16)
    put_mixed = pltpu.make_async_copy(mixed_ref, mixed_h, loc_sem.at[0])
    put_gin = pltpu.make_async_copy(gin_ref, gin_h.at[0], loc_sem.at[1])
    put_gout = pltpu.make_async_copy(go_buf, gout_h.at[0], loc_sem.at[2])
    put_mixed.start()

    def arrived_gin(s):
        p = mate(s)
        arrived(gin_all.at[p], gin_r.at[p])

    each(1, nd, arrived_gin)
    gin_ref[...] = jnp.sum(gin_all[...], axis=0)[:, 0:hidden].astype(BF16)
    put_gin.start()

    def arrived_go(s):
        p = mate(s)

        @pl.when(p < parts)
        def _():
            arrived(go_buf.at[:, cols(p)], go_r.at[p])

    each(1, nd, arrived_go)
    put_gout.start()

    def drain(s):
        gate_copy(s).wait_send()
        lg_copy(s).wait_send()
        rk_copy(peer(s)).wait_send()

        @pl.when(owner)
        def _():
            au_copy(s).wait_send()
            ge_copy(s).wait_send()

    each(1, n, drain)

    def drain_line(z):
        def piece(c):
            @pl.when((z <= at_line) & (at_line + 1 < line))
            def _():
                up_copy(z, c).wait_send()

            @pl.when((z >= at_line) & (at_line >= 1))
            def _():
                down_copy(z, c).wait_send()

            @pl.when(crosses(z))
            def _():
                each(1, side, lambda s: side_copy(z, s, c).wait_send())

            @pl.when((z == at_line) & outer)
            def _():
                each(1, side, lambda s: onward_copy(s, c).wait_send())

            lined = far(at_line, z) | (~outer & (z == at_line - front))

            @pl.when((z == at_line) | lined)
            def _():
                each(1, side, lambda s: pair_copy(z, other(s), c).wait_send())

            @pl.when(lined)
            def _():
                line_copy(z, c).wait_send()

        each(0, CHUNKS, piece)

        @pl.when(z == at_line + front)
        def _():
            each(0, side, lambda x: near_copy(z, x).wait_send())

    each(0, line, drain_line)

    def drain_mates(s):
        gin_copy(s).wait_send()

        @pl.when(mate(s) < parts)
        def _():
            gm_copy(s).wait_send()

        @pl.when(owner)
        def _():
            am_copy(s).wait_send()
            go_copy(s).wait_send()

    each(1, nd, drain_mates)
    put_mixed.wait()
    put_gin.wait()
    put_gout.wait()


def hand_over(a_ref, b_ref, c_ref, x_ref, y_ref, z_ref):
    x_ref[...] = a_ref[...]
    y_ref[...] = b_ref[...]
    z_ref[...] = c_ref[...]


def shards(
    n,
    nd,
    tokens,
    chosen_expert_index,
    router_gate_weight,
    output_gradient,
    gate_weight_matrix,
    up_weight,
    down_weight,
    adapter_down_maps,
    adapter_up_maps,
):
    rows, width = tokens.shape
    rank, hidden = adapter_down_maps.shape[1:]
    line = line_of(n)
    side = n // line
    parts = parts_of(nd, width)
    part = width // parts
    vmem = pl.BlockSpec(memory_space=pltpu.VMEM)
    hbm = pl.BlockSpec(memory_space=pltpu.HBM)
    dma = pltpu.SemaphoreType.DMA
    results = pl.pallas_call(
        functools.partial(kernel, n, nd),
        out_shape=(
            jax.ShapeDtypeStruct((rows, width), BF16),
            jax.ShapeDtypeStruct((1, rank, hidden), BF16),
            jax.ShapeDtypeStruct((1, rank, width), BF16),
        ),
        in_specs=[hbm] * 9,
        out_specs=(hbm,) * 3,
        scratch_shapes=[
            pltpu.VMEM((n, rows, width), BF16),
            pltpu.VMEM(chosen_expert_index.shape[::-1], jnp.int32),
            pltpu.VMEM(router_gate_weight.shape[::-1], F32),
            pltpu.VMEM((rows, width), BF16),
            pltpu.VMEM((rank, hidden), BF16),
            pltpu.VMEM((hidden, width), BF16),
            pltpu.VMEM((hidden, width), BF16),
            pltpu.VMEM((hidden + rank, width), BF16),
            pltpu.VMEM((n, rows, hidden + rank), BF16),
            pltpu.VMEM((n, rows, width), BF16),
            pltpu.VMEM((n, rows, width), BF16),
            pltpu.VMEM((2, side, rows, width), BF16),
            pltpu.VMEM((line, rows, width), BF16),
            pltpu.VMEM((line, rows, width), BF16),
            pltpu.VMEM((n, 1, rows), F32),
            pltpu.VMEM((n, rank, width), BF16),
            pltpu.VMEM((n, rank, rows), BF16),
            pltpu.VMEM((n, rank, rows), BF16),
            pltpu.VMEM((n, rank, rows), BF16),
            pltpu.VMEM((n, rank, rows), BF16),
            pltpu.VMEM((n, rank, rows), F32),
            pltpu.VMEM((n * rank, width), BF16),
            pltpu.VMEM((nd, n * rank, part), BF16),
            pltpu.VMEM((n, rank, part), BF16),
            pltpu.VMEM((n, rank, part), BF16),
            pltpu.VMEM((rank, width), BF16),
            pltpu.VMEM((nd, rank, hidden + rank), F32),
            pltpu.VMEM((rows, width), F32),
            pltpu.VMEM((rows, width), BF16),
            pltpu.VMEM((rank, hidden), BF16),
            pltpu.SemaphoreType.REGULAR((3,)),
            dma((10,)),
        ]
        + [dma((line, CHUNKS))] * 2
        + [dma((n, CHUNKS)), dma((side, CHUNKS))]
        + [dma((n, CHUNKS))] * 3
        + [dma((2, side))] * 2
        + [dma((line, CHUNKS))] * 2
        + [dma((n,))] * 4
        + [dma((nd,))] * 2
        + [dma((n,))] * 4
        + [dma((nd,))] * 2
        + [dma((n,))] * 2
        + [dma((nd,))] * 4,
        compiler_params=pltpu.CompilerParams(
            collective_id=0, has_side_effects=True, vmem_limit_bytes=60 * 1024 * 1024
        ),
    )(
        tokens,
        chosen_expert_index.T,
        router_gate_weight.T,
        output_gradient,
        jnp.swapaxes(gate_weight_matrix, 1, 2),
        jnp.swapaxes(up_weight, 1, 2),
        down_weight,
        adapter_down_maps,
        adapter_up_maps,
    )
    return pl.pallas_call(
        hand_over,
        out_shape=tuple(jax.ShapeDtypeStruct(r.shape, r.dtype) for r in results),
        in_specs=[vmem] * 3,
        out_specs=(vmem,) * 3,
    )(*results)


def solution(mesh):
    return jax.shard_map(
        functools.partial(shards, mesh.shape["expert"], mesh.shape["dp"]),
        mesh=mesh,
        in_specs=(
            P(("dp", "expert"), None),
            P(("dp", "expert"), None),
            P(("dp", "expert"), None),
            P(("dp", "expert"), None),
            P("expert", None, None),
            P("expert", None, None),
            P("expert", None, None),
            P("expert", None, None),
            P("expert", None, None),
        ),
        out_specs=(P(("dp", "expert"), None), P("expert", None, None), P("expert", None, None)),
        check_vma=False,
    )
```
